512 devices in a mesh: pairs: 2 (over y), gx: 32 (over z), gy: 4 (over x), gz: 2 (over core).
Axes of the slice: x: 4, y: 2, z: 32, core: 2. Of those that a mesh axis runs over, the one named last changes fastest.
The devices are a block of a 4x8x32 slice.
Arguments:
- fine_start: float32 [512, 256, 512], P(('pairs', 'gx'), 'gy', 'gz'), parts along dimension 0, may hold values from -1 to 1
- increments: float32 [2, 512, 256, 512], P(None, ('pairs', 'gx'), 'gy', 'gz'), parts along dimension 1, may hold values from -5 to 5
- coarse_start: float32 [256, 128, 256], P(('pairs', 'gx')), parts along dimension 0, may hold values from -1 to 1
Outputs:
- fine_final: float32 [512, 256, 512], P(('pairs', 'gx'), 'gy', 'gz'), parts along dimension 0
- coarse_final: float32 [256, 128, 256], P(('pairs', 'gx')), parts along dimension 0
The draws below stay inside these ranges and needn't reach their ends.
There are 2 independent parts, one for each index of `pairs`. The reference program is written for one: setup_inputs(seed, part) draws one part's arguments, and reference() takes and returns one part's arrays. A program takes and returns all parts, laid end to end along the dimension named above; each array names one. Nothing has to cross between parts.
All inputs are finite; a program needn't handle non-finite values.
Results may differ from the reference program's by a relative error of at most 0.00002.
Values sent between devices are 32-bit elements; how exact they have to be, the bound alone decides.
A program may use at most 128 MiB of HBM per device.

```python
import jax
import jax.numpy as jnp

STEPS = 2
SWEEPS = 2
NX = 256
NY = 256
NZ = 512


def draw_increments(key, part):
    extent = (STEPS, NX, NY, NZ)
    values = jnp.clip(jax.random.normal(key, extent, jnp.float32), -5.0, 5.0)
    return values


def shard_levels(stream_key, shape, shards, least, largest):
    def one(axis_at, blocks):
        steps = jax.random.uniform(jax.random.fold_in(jax.random.fold_in(stream_key, 6), axis_at), (blocks,), jnp.float32, least / len(shards), largest / len(shards))
        return jnp.repeat(jnp.exp(steps), shape[axis_at] // blocks).reshape((-1,) + (1,) * (len(shape) - axis_at - 1))

    gain = one(*shards[0])
    for cut in shards[1:]:
        gain = gain * one(*cut)
    return gain


def setup_inputs(seed: int = 0, part: int = 0) -> dict:
    seeds = jax.random.split(jax.random.key(seed), 4)
    own_keys = jax.random.split(jax.random.fold_in(seeds[3], part), 4)
    fine_start = jnp.clip(jax.random.uniform(own_keys[0], (NX, NY, NZ), jnp.float32, -1.0, 1.0) * shard_levels(own_keys[0], (NX, NY, NZ), ((0, 32), (1, 4), (2, 2)), -0.4, 0.0), -1.0, 1.0)
    increments = draw_increments(jax.random.fold_in(jax.random.fold_in(seeds[3], part), 71), part)
    coarse_start = jnp.clip(jax.random.uniform(own_keys[2], (NX // 2, NY // 2, NZ // 2), jnp.float32, -1.0, 1.0) * shard_levels(own_keys[2], (NX // 2, NY // 2, NZ // 2), ((0, 32),), -0.4, 0.0), -1.0, 1.0)
    return dict(fine_start=fine_start, increments=increments, coarse_start=coarse_start)


noise_scale = 0.3
fine_step = 0.2
coarse_step = 0.4
fine_coupling = 1.0
coarse_coupling = 0.5


def neighbours(padded):
    beside = padded[2:, 1:-1, 1:-1] + padded[:-2, 1:-1, 1:-1]
    beside = beside + padded[1:-1, 2:, 1:-1] + padded[1:-1, :-2, 1:-1]
    beside = beside + padded[1:-1, 1:-1, 2:] + padded[1:-1, 1:-1, :-2]
    return beside


def advance(state, forcing, step_size, coupling):
    source = state + step_size * (state - state * state * state) + noise_scale * forcing
    fields = source
    for sweep_index in range(SWEEPS):
        padded = jnp.pad(fields, 1, mode="wrap")
        fields = (source + coupling * neighbours(padded)) / (1.0 + 6.0 * coupling)
    return fields


def reference(fine_start, increments, coarse_start):
    state = fine_start
    for step_index in range(STEPS):
        state = advance(state, increments[step_index], fine_step, fine_coupling)
    summed = jnp.sum(increments, axis=0)
    coarse_noise = 0.125 * summed.reshape(NX // 2, 2, NY // 2, 2, NZ // 2, 2).sum(axis=(1, 3, 5))
    coarse_final = advance(coarse_start, coarse_noise, coarse_step, coarse_coupling)
    return state, coarse_final
```

```python
import functools

import jax
import jax.numpy as jnp
from jax import lax
from jax.experimental import pallas as pl
from jax.experimental.pallas import tpu as pltpu
from jax.sharding import PartitionSpec as P

MESH = pl.DeviceIdType.MESH
NOISE = 0.3
FINE_STEP = 0.2
COARSE_STEP = 0.4
COARSE_COUPLING = 0.5
FINE_SCALE = 1.0 / 7.0
COARSE_SCALE = 1.0 / 4.0


def reaction(state, forcing, step):
    return state + step * (state - state * state * state) + NOISE * forcing


def ring_sum(center):
    rows, lanes = center.shape
    beside = pltpu.roll(center, rows - 1, 0) + pltpu.roll(center, 1, 0)
    return beside + (pltpu.roll(center, lanes - 1, 1) + pltpu.roll(center, 1, 1))


def kernel(sizes, u_hbm, e_hbm, cs_hbm, fo, co, u, e, cs, v1, v2, w, zs1, zs2, pks, pkr,
           sums, c, cw, cblk, load_sem, send_sem, recv_sem):
    n_gx, n_gy, n_gz = sizes
    X, Y, Z = u.shape
    CX, CY, CZ = cs.shape
    me_x, me_y, me_z = lax.axis_index("gx"), lax.axis_index("gy"), lax.axis_index("gz")
    R, L = lax.rem(me_x + 1, n_gx), lax.rem(me_x + n_gx - 1, n_gx)
    U, D = lax.rem(me_y + 1, n_gy), lax.rem(me_y + n_gy - 1, n_gy)
    O = lax.rem(me_y + 2, n_gy)
    Q = lax.rem(me_z + 1, n_gz)

    def dev(x=None, y=None, z=None):
        return {"gx": me_x if x is None else x, "gy": me_y if y is None else y,
                "gz": me_z if z is None else z}

    loads = []

    def load(src, dst):
        k = len(loads)
        copy = pltpu.make_async_copy(src, dst, load_sem.at[k])
        copy.start()
        loads.append(copy)
        return copy

    lu0, le0 = load(u_hbm.at[0:2], u.at[0:2]), load(e_hbm.at[0, 0:2], e.at[0, 0:2])
    lu3, le3 = load(u_hbm.at[X - 2 : X], u.at[X - 2 : X]), load(e_hbm.at[0, X - 2 : X], e.at[0, X - 2 : X])
    le1 = load(e_hbm.at[1], e.at[1])
    lem = load(e_hbm.at[0, 2 : X - 2], e.at[0, 2 : X - 2])
    own_y = pl.ds(pl.multiple_of(me_y * CY, 8), CY)
    own_z = pl.ds(pl.multiple_of(me_z * CZ, 128), CZ)
    lcs = load(cs_hbm.at[:, own_y, own_z], cs)
    lum = load(u_hbm.at[2 : X - 2], u.at[2 : X - 2])

    barrier = pltpu.get_barrier_semaphore()
    partners = [dev(x=R), dev(x=L), dev(x=R, z=Q), dev(x=L, z=Q),
                dev(x=R, y=U), dev(x=R, y=D), dev(x=L, y=U), dev(x=L, y=D),
                dev(y=U), dev(y=D), dev(y=U, z=Q), dev(y=D, z=Q), dev(z=Q), dev(y=O)]
    for partner in partners:
        pl.semaphore_signal(barrier, inc=1, device_id=partner, device_id_type=MESH)

    sends = []

    def send(src, dst, to):
        k = len(sends)
        copy = pltpu.make_async_remote_copy(
            src_ref=src, dst_ref=dst, send_sem=send_sem.at[k], recv_sem=recv_sem.at[k],
            device_id=to, device_id_type=MESH)
        copy.start()
        sends.append(copy)
        return copy

    lane = lax.broadcasted_iota(jnp.int32, (Y, 128), 1)

    def first_advance(x):
        v1[2 + x, 0:Y, 0:Z] = reaction(u[x], e[0, x], FINE_STEP)

    def z_select(v, zs, x):
        zs[x] = jnp.where(lane < 64, v[2 + x, 0:Y, 0:128], v[2 + x, 0:Y, Z - 128 : Z])

    def pack(v, slot):
        columns = [
            jnp.where(lane == 0, v[2 + x, 0:Y, 0:128], pltpu.roll(v[2 + x, 0:Y, Z - 128 : Z], 8, 1))
            for x in (0, X - 1)
        ]
        pks[slot] = jnp.transpose(jnp.concatenate(columns, axis=0))[0:8, :]

    def unpack(v, slot):
        from_left = jnp.transpose(jnp.concatenate([pkr[slot, 0]] * 16, axis=0))
        from_right = jnp.transpose(jnp.concatenate([pkr[slot, 1]] * 16, axis=0))
        v[1, 0:Y, Z : Z + 128] = from_left[Y : 2 * Y, :]
        v[X + 2, 0:Y, Z : Z + 128] = from_right[0:Y, :]

    def send_near(v):
        return [send(v.at[X + 1, 0:Y, 0:Z], v.at[1, 0:Y, 0:Z], dev(x=R)),
                send(v.at[2, 0:Y, 0:Z], v.at[X + 2, 0:Y, 0:Z], dev(x=L))]

    def send_far(v):
        return [send(v.at[X, 0:Y, 0:Z], v.at[0, 0:Y, 0:Z], dev(x=R)),
                send(v.at[3, 0:Y, 0:Z], v.at[X + 3, 0:Y, 0:Z], dev(x=L))]

    def send_diagonals(v, slot):
        out = []
        for mine, theirs, x in ((X + 1, 1, R), (2, X + 2, L)):
            out.append(send(v.at[mine, Y - 1 : Y, 0:Z], v.at[theirs, Y + 7 : Y + 8, 0:Z], dev(x=x, y=U)))
            out.append(send(v.at[mine, 0:1, 0:Z], v.at[theirs, Y : Y + 1, 0:Z], dev(x=x, y=D)))
        out.append(send(pks.at[slot], pkr.at[slot, 0], dev(x=R, z=Q)))
        out.append(send(pks.at[slot], pkr.at[slot, 1], dev(x=L, z=Q)))
        return out

    def send_sides(v, zs, first, last):
        xs, ext = slice(first, last), slice(first + 2, last + 2)
        return [
            send(zs.at[xs], v.at[ext, 0:Y, Z : Z + 128], dev(z=Q)),
            send(v.at[ext, Y - 2 : Y, 0:Z], v.at[ext, Y + 6 : Y + 8, 0:Z], dev(y=U)),
            send(v.at[ext, 0:2, 0:Z], v.at[ext, Y : Y + 2, 0:Z], dev(y=D)),
            send(zs.at[xs, Y - 2 : Y], v.at[ext, Y + 6 : Y + 8, Z : Z + 128], dev(y=U, z=Q)),
            send(zs.at[xs, 0:2], v.at[ext, Y : Y + 2, Z : Z + 128], dev(y=D, z=Q)),
        ]

    def wait(copies):
        for copy in copies:
            copy.wait_recv()

    def sweep_one(v, k):
        center = v[k]
        w[k - 1] = (center + (v[k + 1] + v[k - 1] + ring_sum(center))) * FINE_SCALE

    def sweep_one_own(v, k):
        center = v[k]
        beside = v[k + 1, 0:Y, 0:Z] + v[k - 1, 0:Y, 0:Z] + ring_sum(center)[0:Y, 0:Z]
        w[k - 1, 0:Y, 0:Z] = (center[0:Y, 0:Z] + beside) * FINE_SCALE

    def sweep_two(v, k):
        beside = w[k, 0:Y, 0:Z] + w[k - 2, 0:Y, 0:Z] + ring_sum(w[k - 1])[0:Y, 0:Z]
        return (v[k, 0:Y, 0:Z] + beside) * FINE_SCALE

    def second_advance(k):
        v2[k, 0:Y, 0:Z] = reaction(sweep_two(v1, k), e[1, k - 2], FINE_STEP)

    def planes(first, last, body):
        def step(k, carry):
            body(k)
            return carry
        lax.fori_loop(first, last, step, 0)

    lu0.wait()
    le0.wait()
    first_advance(0)
    lu3.wait()
    le3.wait()
    first_advance(X - 1)
    pl.semaphore_wait(barrier, len(partners))
    near1 = send_near(v1)

    le1.wait()
    lem.wait()
    for x in range(CX):
        total = (e[0, 2 * x] + e[0, 2 * x + 1]) + (e[1, 2 * x] + e[1, 2 * x + 1])
        for t in range(Z // 128):
            sums[t, x * Y : (x + 1) * Y, :] = total[:, t * 128 : (t + 1) * 128]
    pairs = [sums[t, pl.ds(0, CX * CY, stride=2), :] + sums[t, pl.ds(1, CX * CY, stride=2), :]
             for t in range(Z // 128)]
    halve = (lax.broadcasted_iota(jnp.int32, (Z, CZ), 0) // 2
             == lax.broadcasted_iota(jnp.int32, (Z, CZ), 1)).astype(jnp.float32)
    noise = 0.125 * jnp.dot(jnp.concatenate(pairs, axis=1), halve,
                            precision=lax.Precision.HIGHEST, preferred_element_type=jnp.float32)
    lcs.wait()
    c[2 : CX + 2, 0:CY, 0:CZ] = reaction(cs[...], noise.reshape(CX, CY, CZ), COARSE_STEP)
    coarse_x = [
        send(c.at[CX : CX + 2, 0:CY, 0:CZ], c.at[0:2, 0:CY, 0:CZ], dev(x=R)),
        send(c.at[2:4, 0:CY, 0:CZ], c.at[CX + 2 : CX + 4, 0:CY, 0:CZ], dev(x=L)),
        send(c.at[CX + 1, 0:CY, 0:CZ], c.at[1, 0:CY, CZ : 2 * CZ], dev(x=R, z=Q)),
        send(c.at[2, 0:CY, 0:CZ], c.at[CX + 2, 0:CY, CZ : 2 * CZ], dev(x=L, z=Q)),
    ]
    for mine, theirs, x in ((CX + 1, 1, R), (2, CX + 2, L)):
        coarse_x.append(send(c.at[mine, CY - 1 : CY, 0:CZ], c.at[theirs, CY + 7 : CY + 8, 0:CZ], dev(x=x, y=U)))
        coarse_x.append(send(c.at[mine, 0:1, 0:CZ], c.at[theirs, CY : CY + 1, 0:CZ], dev(x=x, y=D)))
    inner = slice(2, CX + 2)
    coarse_yz = [
        send(c.at[inner, 0:CY, 0:CZ], c.at[inner, 0:CY, CZ : 2 * CZ], dev(z=Q)),
        send(c.at[inner, CY - 2 : CY, 0:CZ], c.at[inner, CY + 6 : CY + 8, 0:CZ], dev(y=U)),
        send(c.at[inner, 0:2, 0:CZ], c.at[inner, CY : CY + 2, 0:CZ], dev(y=D)),
        send(c.at[inner, CY - 1 : CY, 0:CZ], c.at[inner, CY + 7 : CY + 8, CZ : 2 * CZ], dev(y=U, z=Q)),
        send(c.at[inner, 0:1, 0:CZ], c.at[inner, CY : CY + 1, CZ : 2 * CZ], dev(y=D, z=Q)),
    ]

    first_advance(1)
    first_advance(X - 2)
    far1 = send_far(v1)
    pack(v1, 0)
    diag1 = send_diagonals(v1, 0)
    lum.wait()
    planes(2, X - 2, first_advance)
    planes(0, X, lambda x: z_select(v1, zs1, x))
    sides1 = send_sides(v1, zs1, 0, X)

    wait(sides1)
    planes(3, X + 1, lambda k: sweep_one(v1, k))
    planes(4, X, second_advance)

    wait(near1)
    for k in (2, X + 1):
        sweep_one_own(v1, k)
    for k in (3, X):
        second_advance(k)
    far2 = send_far(v2)
    planes(1, X - 1, lambda x: z_select(v2, zs2, x))
    inside2 = send_sides(v2, zs2, 1, X - 1)

    wait(coarse_yz)
    wait(coarse_x)
    for k in range(1, CX + 3):
        center = c[k]
        beside = c[k + 1] + c[k - 1] + ring_sum(center)
        cw[k - 1] = (center + COARSE_COUPLING * beside) * COARSE_SCALE
    for k in range(2, CX + 2):
        beside = cw[k, 0:CY, 0:CZ] + cw[k - 2, 0:CY, 0:CZ] + ring_sum(cw[k - 1])[0:CY, 0:CZ]
        cblk[k - 2] = (c[k, 0:CY, 0:CZ] + COARSE_COUPLING * beside) * COARSE_SCALE
    mine = co.at[:, own_y, own_z]
    gather = [send(cblk, mine, dev(y=O)), send(cblk, mine, dev(y=U)), send(cblk, mine, dev(y=D))]
    direct = send(cblk, mine, dev(z=Q))
    co[:, own_y, own_z] = cblk[...]

    wait(far1)
    wait(diag1)
    unpack(v1, 0)
    for k in (1, X + 2):
        sweep_one_own(v1, k)
    for k in (2, X + 1):
        sweep_one(v1, k)
    for k in (2, X + 1):
        second_advance(k)
    near2 = send_near(v2)
    pack(v2, 1)
    diag2 = send_diagonals(v2, 1)
    z_select(v2, zs2, 0)
    z_select(v2, zs2, X - 1)
    outside2 = send_sides(v2, zs2, 0, 1) + send_sides(v2, zs2, X - 1, X)

    wait(inside2)
    planes(4, X, lambda k: sweep_one(v2, k))

    def finish(k):
        fo[k - 2] = sweep_two(v2, k)

    planes(5, X - 1, finish)

    passed = []
    for copy, owner in ((gather[1], D), (gather[2], U), (gather[0], O)):
        copy.wait_recv()
        block = co.at[:, pl.ds(pl.multiple_of(owner * CY, 8), CY), own_z]
        passed.append(send(block, block, dev(z=Q)))

    wait(outside2)
    for k in (3, X):
        sweep_one(v2, k)
    for k in (4, X - 1):
        finish(k)
    wait(far2)
    wait(near2)
    wait(diag2)
    unpack(v2, 1)
    for k in (1, X + 2):
        sweep_one_own(v2, k)
    for k in (2, X + 1):
        sweep_one(v2, k)
    for k in (2, 3, X, X + 1):
        finish(k)

    direct.wait_recv()
    wait(passed)
    for copy in sends:
        copy.wait_send()


N_MESSAGES = 64


def body(sizes, fine_start, increments, coarse_start):
    X, Y, Z = fine_start.shape
    CX, CY, CZ = X // 2, Y // 2, Z // 2
    f32 = jnp.float32
    any_space = pl.BlockSpec(memory_space=pl.ANY)
    in_vmem = pl.BlockSpec(memory_space=pltpu.VMEM)
    fine, coarse = pl.pallas_call(
        functools.partial(kernel, sizes),
        out_shape=(pltpu.VMEM((X, Y, Z), f32), pltpu.VMEM(coarse_start.shape, f32)),
        in_specs=[any_space] * 3,
        out_specs=(in_vmem, in_vmem),
        scratch_shapes=[
            pltpu.VMEM((X, Y, Z), f32),
            pltpu.VMEM((2, X, Y, Z), f32),
            pltpu.VMEM((CX, CY, CZ), f32),
            pltpu.VMEM((X + 4, Y + 8, Z + 128), f32),
            pltpu.VMEM((X + 4, Y + 8, Z + 128), f32),
            pltpu.VMEM((X + 2, Y + 8, Z + 128), f32),
            pltpu.VMEM((X, Y, 128), f32),
            pltpu.VMEM((X, Y, 128), f32),
            pltpu.VMEM((2, 8, 128), f32),
            pltpu.VMEM((2, 2, 8, 128), f32),
            pltpu.VMEM((Z // 128, CX * Y, 128), f32),
            pltpu.VMEM((CX + 4, CY + 8, 2 * CZ), f32),
            pltpu.VMEM((CX + 2, CY + 8, 2 * CZ), f32),
            pltpu.VMEM((CX, CY, CZ), f32),
            pltpu.SemaphoreType.DMA((8,)),
            pltpu.SemaphoreType.DMA((N_MESSAGES,)),
            pltpu.SemaphoreType.DMA((N_MESSAGES,)),
        ],
        compiler_params=pltpu.CompilerParams(collective_id=0, has_side_effects=True),
    )(fine_start, increments, coarse_start)
    return fine, coarse


def solution(mesh):
    sizes = tuple(mesh.shape[name] for name in ("gx", "gy", "gz"))
    return jax.shard_map(
        functools.partial(body, sizes),
        mesh=mesh,
        in_specs=(
            P(("pairs", "gx"), "gy", "gz"),
            P(None, ("pairs", "gx"), "gy", "gz"),
            P(("pairs", "gx"), None, None),
        ),
        out_specs=(P(("pairs", "gx"), "gy", "gz"), P(("pairs", "gx"), None, None)),
        check_vma=False,
    )
```

```python
import functools

import jax
import jax.numpy as jnp
from jax import lax
from jax.experimental import pallas as pl
from jax.experimental.pallas import tpu as pltpu
from jax.sharding import PartitionSpec as P

MESH = pl.DeviceIdType.MESH
NOISE = 0.3
FINE_STEP = 0.2
COARSE_STEP = 0.4
COARSE_COUPLING = 0.5
S = 1.0 / 7.0
COARSE_SCALE = 1.0 / 4.0


def reaction(state, forcing, step):
    return state + step * (state - state * state * state) + NOISE * forcing


def ring_sum(center):
    rows, lanes = center.shape
    beside = pltpu.roll(center, rows - 1, 0) + pltpu.roll(center, 1, 0)
    return beside + (pltpu.roll(center, lanes - 1, 1) + pltpu.roll(center, 1, 1))


def kernel(sizes, u_hbm, e_hbm, cs_hbm, fo, co, u, e, cs, v1, v2, w, p0, k0, k1, zs1, zs2, pks, pkr,
           sums, c, cw, cblk, load_sem, send_sem, recv_sem):
    n_gx, n_gy, n_gz = sizes
    X, Y, Z = u.shape
    CX, CY, CZ = cs.shape
    me_x, me_y, me_z = lax.axis_index("gx"), lax.axis_index("gy"), lax.axis_index("gz")
    R, L = lax.rem(me_x + 1, n_gx), lax.rem(me_x + n_gx - 1, n_gx)
    U, D = lax.rem(me_y + 1, n_gy), lax.rem(me_y + n_gy - 1, n_gy)
    O = lax.rem(me_y + 2, n_gy)
    Q = lax.rem(me_z + 1, n_gz)
    one, zero, near, far = (0, X - 3), (X - 2, X - 1), (X, X + 1), (X + 2, X + 3)
    two = (1, X - 4)
    place = {0: X - 2, X - 1: X - 1}
    place.update({x: x - 1 for x in range(1, X - 1)})
    rows, lanes = slice(0, Y), slice(0, Z)

    def dev(x=None, y=None, z=None):
        return {"gx": me_x if x is None else x, "gy": me_y if y is None else y,
                "gz": me_z if z is None else z}

    loads = []

    def load(src, dst):
        copy = pltpu.make_async_copy(src, dst, load_sem.at[len(loads)])
        copy.start()
        loads.append(copy)
        return copy

    own_y = pl.ds(pl.multiple_of(me_y * CY, 8), CY)
    own_z = pl.ds(pl.multiple_of(me_z * CZ, 128), CZ)
    first = [load(u_hbm.at[0:2], u.at[0:2]), load(e_hbm.at[0, 0:2], e.at[0, 0:2]),
             load(u_hbm.at[X - 2 : X], u.at[X - 2 : X]),
             load(e_hbm.at[0, X - 2 : X], e.at[0, X - 2 : X])]
    second = [load(e_hbm.at[1], e.at[1]), load(e_hbm.at[0, 2 : X - 2], e.at[0, 2 : X - 2]),
              load(cs_hbm.at[:, own_y, own_z], cs)]
    third = load(u_hbm.at[2 : X - 2], u.at[2 : X - 2])

    barrier = pltpu.get_barrier_semaphore()
    partners = [dev(x=R, y=U), dev(x=R, y=D), dev(x=L, y=U), dev(x=L, y=D), dev(y=O),
                dev(x=R, z=Q), dev(x=L, z=Q), dev(x=R), dev(x=L),
                dev(y=U, z=Q), dev(y=D, z=Q), dev(y=U), dev(y=D), dev(z=Q)]
    for partner in partners:
        pl.semaphore_signal(barrier, inc=1, device_id=partner, device_id_type=MESH)

    sends = []

    def send(src, dst, to):
        k = len(sends)
        copy = pltpu.make_async_remote_copy(
            src_ref=src, dst_ref=dst, send_sem=send_sem.at[k], recv_sem=recv_sem.at[k],
            device_id=to, device_id_type=MESH)
        copy.start()
        sends.append(copy)
        return copy

    def wait(copies):
        for copy in copies:
            copy.wait_recv()

    def planes(start, stop, step_body):
        def step(k, carry):
            step_body(k)
            return carry
        lax.fori_loop(start, stop, step, 0)

    lane = lax.broadcasted_iota(jnp.int32, (Y, 128), 1)
    coarse_lane = lax.broadcasted_iota(jnp.int32, (CY, 128), 1)

    def first_advance(x, at):
        v1[at, rows, lanes] = reaction(u[x], e[0, x], FINE_STEP)

    def z_select(v, zs, k):
        zs[k] = jnp.where(lane < 64, v[k, rows, 0:128], v[k, rows, Z - 128 : Z])

    def pack(v, slot):
        columns = [jnp.where(lane == 0, v[k, rows, 0:128], pltpu.roll(v[k, rows, Z - 128 : Z], 8, 1))
                   for k in zero]
        pks[slot] = jnp.transpose(jnp.concatenate(columns, axis=0))[0:8, :]

    def unpacked(slot, side):
        return jnp.transpose(jnp.concatenate([pkr[slot, side]] * 16, axis=0))

    def unpack(v, slot):
        v[near[0], rows, Z : Z + 128] = unpacked(slot, 0)[Y : 2 * Y, :]
        v[near[1], rows, Z : Z + 128] = unpacked(slot, 1)[0:Y, :]

    def send_near(v):
        return [send(v.at[zero[1], rows, lanes], v.at[near[0], rows, lanes], dev(x=R)),
                send(v.at[zero[0], rows, lanes], v.at[near[1], rows, lanes], dev(x=L))]

    def send_far(v):
        return [send(v.at[one[1], rows, lanes], v.at[far[0], rows, lanes], dev(x=R)),
                send(v.at[one[0], rows, lanes], v.at[far[1], rows, lanes], dev(x=L))]

    def send_corner_rows(v):
        out = []
        for mine, theirs, x in ((zero[1], near[0], R), (zero[0], near[1], L)):
            out.append(send(v.at[mine, Y - 1 : Y, lanes], v.at[theirs, Y + 7 : Y + 8, lanes], dev(x=x, y=U)))
            out.append(send(v.at[mine, 0:1, lanes], v.at[theirs, Y : Y + 1, lanes], dev(x=x, y=D)))
        return out

    def send_packed(slot):
        return [send(pks.at[slot], pkr.at[slot, 0], dev(x=R, z=Q)),
                send(pks.at[slot], pkr.at[slot, 1], dev(x=L, z=Q))]

    def send_sides(v, zs, start, stop):
        ks = slice(start, stop)
        ring = slice(Z, Z + 128)
        return [
            send(v.at[ks, Y - 2 : Y, lanes], v.at[ks, Y + 6 : Y + 8, lanes], dev(y=U)),
            send(v.at[ks, 0:2, lanes], v.at[ks, Y : Y + 2, lanes], dev(y=D)),
            send(zs.at[ks, Y - 2 : Y], v.at[ks, Y + 6 : Y + 8, ring], dev(y=U, z=Q)),
            send(zs.at[ks, 0:2], v.at[ks, Y : Y + 2, ring], dev(y=D, z=Q)),
            send(zs.at[ks], v.at[ks, rows, ring], dev(z=Q)),
        ]

    def sweep_one(v, k, below, above):
        center = v[k]
        w[k] = (center + (v[above] + v[below] + ring_sum(center))) * S

    def partial_two(v, k, above):
        return v[k, rows, lanes] + (w[above, rows, lanes] + ring_sum(w[k])[rows, lanes])

    def sweep_two(v, k, below, above):
        return (partial_two(v, k, above) + w[below, rows, lanes]) * S

    for copy in first:
        copy.wait()
    for x in (0, X - 1, 1, X - 2):
        first_advance(x, place[x])
    for copy in second:
        copy.wait()
    for x in range(CX):
        total = (e[0, 2 * x] + e[0, 2 * x + 1]) + (e[1, 2 * x] + e[1, 2 * x + 1])
        for t in range(Z // 128):
            sums[t, x * Y : (x + 1) * Y, :] = total[:, t * 128 : (t + 1) * 128]
    pairs = [sums[t, pl.ds(0, CX * CY, stride=2), :] + sums[t, pl.ds(1, CX * CY, stride=2), :]
             for t in range(Z // 128)]
    halve = (lax.broadcasted_iota(jnp.int32, (Z, CZ), 0) // 2
             == lax.broadcasted_iota(jnp.int32, (Z, CZ), 1)).astype(jnp.float32)
    noise = 0.125 * jnp.dot(jnp.concatenate(pairs, axis=1), halve,
                            precision=lax.Precision.HIGHEST, preferred_element_type=jnp.float32)
    c[2 : CX + 2, 0:CY, 0:CZ] = reaction(cs[...], noise.reshape(CX, CY, CZ), COARSE_STEP)
    columns = [jnp.where(coarse_lane == 0, c[k, 0:CY, 0:CZ], pltpu.roll(c[k, 0:CY, 0:CZ], 8, 1))
               for k in (2, CX + 1)]
    pks[2] = jnp.transpose(jnp.concatenate(columns * 2, axis=0))[0:8, :]
    pack(v1, 0)

    pl.semaphore_wait(barrier, len(partners))
    inner = slice(2, CX + 2)
    coarse = []
    for mine, theirs, x in ((CX + 1, 1, R), (2, CX + 2, L)):
        coarse.append(send(c.at[mine, CY - 1 : CY, 0:CZ], c.at[theirs, CY + 7 : CY + 8, 0:CZ], dev(x=x, y=U)))
        coarse.append(send(c.at[mine, 0:1, 0:CZ], c.at[theirs, CY : CY + 1, 0:CZ], dev(x=x, y=D)))
    coarse += [
        send(c.at[CX : CX + 2, 0:CY, 0:CZ], c.at[0:2, 0:CY, 0:CZ], dev(x=R)),
        send(c.at[2:4, 0:CY, 0:CZ], c.at[CX + 2 : CX + 4, 0:CY, 0:CZ], dev(x=L)),
    ]
    coarse += send_packed(2)
    near1 = send_near(v1)
    corner1 = send_corner_rows(v1) + send_packed(0)
    far1 = send_far(v1)
    coarse += [
        send(c.at[inner, CY - 2 : CY, 0:CZ], c.at[inner, CY + 6 : CY + 8, 0:CZ], dev(y=U)),
        send(c.at[inner, 0:2, 0:CZ], c.at[inner, CY : CY + 2, 0:CZ], dev(y=D)),
        send(c.at[inner, CY - 1 : CY, 0:CZ], c.at[inner, CY + 7 : CY + 8, CZ : 2 * CZ], dev(y=U, z=Q)),
        send(c.at[inner, 0:1, 0:CZ], c.at[inner, CY : CY + 1, CZ : 2 * CZ], dev(y=D, z=Q)),
        send(c.at[inner, 0:CY, 0:CZ], c.at[inner, 0:CY, CZ : 2 * CZ], dev(z=Q)),
    ]
    third.wait()
    planes(2, X - 2, lambda x: first_advance(x, x - 1))
    planes(0, X, lambda k: z_select(v1, zs1, k))
    sides1 = send_sides(v1, zs1, 0, X)

    wait(sides1)
    planes(1, X - 3, lambda k: sweep_one(v1, k, k - 1, k + 1))
    for s in range(2):
        sweep_one(v1, one[s], zero[s], two[s])
        center = v1[zero[s]]
        p0[s] = center + (v1[one[s]] + ring_sum(center))
    for s in range(2):
        k1[s] = partial_two(v1, one[s], two[s])

    def second_advance(k):
        v2[k, rows, lanes] = reaction(sweep_two(v1, k, k - 1, k + 1), e[1, k + 1], FINE_STEP)

    planes(1, X - 3, second_advance)

    wait(coarse)
    c[1, 0:CY, CZ : 2 * CZ] = unpacked(2, 0)[CY : 2 * CY, :]
    c[CX + 2, 0:CY, CZ : 2 * CZ] = unpacked(2, 1)[0:CY, :]
    for k in range(1, CX + 3):
        center = c[k]
        beside = c[k + 1] + c[k - 1] + ring_sum(center)
        cw[k - 1] = (center + COARSE_COUPLING * beside) * COARSE_SCALE
    for k in range(2, CX + 2):
        beside = cw[k, 0:CY, 0:CZ] + cw[k - 2, 0:CY, 0:CZ] + ring_sum(cw[k - 1])[0:CY, 0:CZ]
        cblk[k - 2] = (c[k, 0:CY, 0:CZ] + COARSE_COUPLING * beside) * COARSE_SCALE
    mine = co.at[:, own_y, own_z]
    gather = [send(cblk, mine, dev(y=O)), send(cblk, mine, dev(y=U)), send(cblk, mine, dev(y=D))]
    direct = send(cblk, mine, dev(z=Q))
    co[:, own_y, own_z] = cblk[...]

    ends = (0, X - 1)
    nexts = (1, X - 2)
    wait(near1)
    for s in range(2):
        outer = (p0[s, rows, lanes] + v1[near[s], rows, lanes]) * S
        v2[one[s], rows, lanes] = reaction((k1[s] + outer) * S, e[1, nexts[s]], FINE_STEP)
    far2 = send_far(v2)
    planes(0, X - 2, lambda k: z_select(v2, zs2, k))
    inside2 = send_sides(v2, zs2, 0, X - 2)

    wait(corner1)
    unpack(v1, 0)
    for s in range(2):
        outside = v1[near[s]]
        w[zero[s]] = (p0[s] + outside) * S
        beyond = (outside + ring_sum(outside))[rows, lanes] + v1[zero[s], rows, lanes]
        k0[s] = partial_two(v1, zero[s], one[s]) + beyond * S
    wait(far1)
    for s in range(2):
        total = (k0[s] + v1[far[s], rows, lanes] * S) * S
        v2[zero[s], rows, lanes] = reaction(total, e[1, ends[s]], FINE_STEP)
    corner2 = send_corner_rows(v2)
    near2 = send_near(v2)
    pack(v2, 1)
    corner2 += send_packed(1)
    for k in zero:
        z_select(v2, zs2, k)
    outside2 = send_sides(v2, zs2, X - 2, X)

    wait(inside2)
    planes(1, X - 3, lambda k: sweep_one(v2, k, k - 1, k + 1))

    def finish(k):
        fo[k + 1] = sweep_two(v2, k, k - 1, k + 1)

    planes(2, X - 4, finish)

    passed = []

    def pass_on(copy, owner):
        copy.wait_recv()
        block = co.at[:, pl.ds(pl.multiple_of(owner * CY, 8), CY), own_z]
        passed.append(send(block, block, dev(z=Q)))

    pass_on(gather[1], D)
    pass_on(gather[2], U)

    wait(outside2)
    three = (2, X - 5)
    for s in range(2):
        sweep_one(v2, one[s], zero[s], two[s])
        center = v2[zero[s]]
        p0[s] = center + (v2[one[s]] + ring_sum(center))
    for s in range(2):
        fo[place_of(two[s], X)] = sweep_two(v2, two[s], one[s], three[s])
        k1[s] = partial_two(v2, one[s], two[s]) + p0[s, rows, lanes] * S
        k0[s] = (v2[zero[s], rows, lanes] + w[one[s], rows, lanes]
                 + (ring_sum(p0[s])[rows, lanes] + v2[zero[s], rows, lanes]) * S)
    pass_on(gather[0], O)
    wait(far2)
    for s in range(2):
        k0[s] = k0[s] + v2[far[s], rows, lanes] * S
    wait(corner2)
    unpack(v2, 1)
    wait(near2)
    for s in range(2):
        outside = v2[near[s]]
        middle = outside[rows, lanes]
        fo[nexts[s]] = (k1[s] + middle * S) * S
        fo[ends[s]] = (k0[s] + (2.0 * ring_sum(outside)[rows, lanes] + middle) * S) * S

    direct.wait_recv()
    wait(passed)
    for copy in sends:
        copy.wait_send()


def place_of(k, X):
    return k + 1


def write_out(fine, coarse, fine_hbm, coarse_hbm, sems):
    copies = []
    for src, dst in ((fine, fine_hbm), (coarse, coarse_hbm)):
        half = src.shape[0] // 2
        for k in range(2):
            part = slice(k * half, (k + 1) * half)
            copies.append(pltpu.make_async_copy(src.at[part], dst.at[part], sems.at[len(copies)]))
    for copy in copies:
        copy.start()
    for copy in copies:
        copy.wait()


N_MESSAGES = 64


def body(sizes, fine_start, increments, coarse_start):
    X, Y, Z = fine_start.shape
    CX, CY, CZ = X // 2, Y // 2, Z // 2
    f32 = jnp.float32
    any_space = pl.BlockSpec(memory_space=pl.ANY)
    in_vmem = pl.BlockSpec(memory_space=pltpu.VMEM)
    fine, coarse = pl.pallas_call(
        functools.partial(kernel, sizes),
        out_shape=(pltpu.VMEM((X, Y, Z), f32), pltpu.VMEM(coarse_start.shape, f32)),
        in_specs=[any_space] * 3,
        out_specs=(in_vmem, in_vmem),
        scratch_shapes=[
            pltpu.VMEM((X, Y, Z), f32),
            pltpu.VMEM((2, X, Y, Z), f32),
            pltpu.VMEM((CX, CY, CZ), f32),
            pltpu.VMEM((X + 4, Y + 8, Z + 128), f32),
            pltpu.VMEM((X + 4, Y + 8, Z + 128), f32),
            pltpu.VMEM((X, Y + 8, Z + 128), f32),
            pltpu.VMEM((2, Y + 8, Z + 128), f32),
            pltpu.VMEM((2, Y, Z), f32),
            pltpu.VMEM((2, Y, Z), f32),
            pltpu.VMEM((X, Y, 128), f32),
            pltpu.VMEM((X, Y, 128), f32),
            pltpu.VMEM((3, 8, 128), f32),
            pltpu.VMEM((3, 2, 8, 128), f32),
            pltpu.VMEM((Z // 128, CX * Y, 128), f32),
            pltpu.VMEM((CX + 4, CY + 8, 2 * CZ), f32),
            pltpu.VMEM((CX + 2, CY + 8, 2 * CZ), f32),
            pltpu.VMEM((CX, CY, CZ), f32),
            pltpu.SemaphoreType.DMA((8,)),
            pltpu.SemaphoreType.DMA((N_MESSAGES,)),
            pltpu.SemaphoreType.DMA((N_MESSAGES,)),
        ],
        compiler_params=pltpu.CompilerParams(collective_id=0, has_side_effects=True),
    )(fine_start, increments, coarse_start)
    fine = pltpu.with_memory_space_constraint(fine, pltpu.VMEM)
    coarse = pltpu.with_memory_space_constraint(coarse, pltpu.VMEM)
    return pl.pallas_call(
        write_out,
        out_shape=(jax.ShapeDtypeStruct(fine_start.shape, f32),
                   jax.ShapeDtypeStruct(coarse_start.shape, f32)),
        in_specs=[in_vmem, in_vmem],
        out_specs=(any_space, any_space),
        scratch_shapes=[pltpu.SemaphoreType.DMA((4,))],
    )(fine, coarse)


def solution(mesh):
    sizes = tuple(mesh.shape[name] for name in ("gx", "gy", "gz"))
    return jax.shard_map(
        functools.partial(body, sizes),
        mesh=mesh,
        in_specs=(
            P(("pairs", "gx"), "gy", "gz"),
            P(None, ("pairs", "gx"), "gy", "gz"),
            P(("pairs", "gx"), None, None),
        ),
        out_specs=(P(("pairs", "gx"), "gy", "gz"), P(("pairs", "gx"), None, None)),
        check_vma=False,
    )
```

```python
import functools

import jax
import jax.numpy as jnp
from jax import lax
from jax.experimental import pallas as pl
from jax.experimental.pallas import tpu as pltpu
from jax.sharding import PartitionSpec as P

MESH = pl.DeviceIdType.MESH
NOISE = 0.3
FINE_STEP = 0.2
COARSE_STEP = 0.4
COARSE_COUPLING = 0.5
S = 1.0 / 7.0
COARSE_SCALE = 1.0 / 4.0


def reaction(state, forcing, step):
    return state + step * (state - state * state * state) + NOISE * forcing


def ring_sum(center):
    rows, lanes = center.shape
    beside = pltpu.roll(center, rows - 1, 0) + pltpu.roll(center, 1, 0)
    return beside + (pltpu.roll(center, lanes - 1, 1) + pltpu.roll(center, 1, 1))


def kernel(sizes, u_hbm, e_hbm, cs_hbm, fo, co, u, e, cs, v1, v2, w, p0, k0, k1, zs1, zs2, pks, pkr,
           sums, c, cw, cblk, load_sem, send_sem, recv_sem):
    n_gx, n_gy, n_gz = sizes
    X, Y, Z = u.shape
    CX, CY, CZ = cs.shape
    me_x, me_y, me_z = lax.axis_index("gx"), lax.axis_index("gy"), lax.axis_index("gz")
    R, L = lax.rem(me_x + 1, n_gx), lax.rem(me_x + n_gx - 1, n_gx)
    U, D = lax.rem(me_y + 1, n_gy), lax.rem(me_y + n_gy - 1, n_gy)
    O = lax.rem(me_y + 2, n_gy)
    Q = lax.rem(me_z + 1, n_gz)
    one, zero, near, far = (0, X - 3), (X - 2, X - 1), (X, X + 1), (X + 2, X + 3)
    two = (1, X - 4)
    place = {0: X - 2, X - 1: X - 1}
    place.update({x: x - 1 for x in range(1, X - 1)})
    rows, lanes = slice(0, Y), slice(0, Z)

    def dev(x=None, y=None, z=None):
        return {"gx": me_x if x is None else x, "gy": me_y if y is None else y,
                "gz": me_z if z is None else z}

    loads = []

    def load(src, dst):
        copy = pltpu.make_async_copy(src, dst, load_sem.at[len(loads)])
        copy.start()
        loads.append(copy)
        return copy

    own_y = pl.ds(pl.multiple_of(me_y * CY, 8), CY)
    own_z = pl.ds(pl.multiple_of(me_z * CZ, 128), CZ)
    first = [load(u_hbm.at[0:2], u.at[0:2]), load(e_hbm.at[0, 0:2], e.at[0, 0:2]),
             load(u_hbm.at[X - 2 : X], u.at[X - 2 : X]),
             load(e_hbm.at[0, X - 2 : X], e.at[0, X - 2 : X])]
    second = [load(e_hbm.at[1], e.at[1]), load(e_hbm.at[0, 2 : X - 2], e.at[0, 2 : X - 2]),
              load(cs_hbm.at[:, own_y, own_z], cs)]
    third = load(u_hbm.at[2 : X - 2], u.at[2 : X - 2])

    barrier = pltpu.get_barrier_semaphore()
    partners = [dev(x=R, y=U), dev(x=R, y=D), dev(x=L, y=U), dev(x=L, y=D), dev(y=O),
                dev(x=R, z=Q), dev(x=L, z=Q), dev(x=R), dev(x=L),
                dev(y=U, z=Q), dev(y=D, z=Q), dev(y=U), dev(y=D), dev(z=Q)]
    for partner in partners:
        pl.semaphore_signal(barrier, inc=1, device_id=partner, device_id_type=MESH)

    sends = []

    def send(src, dst, to):
        k = len(sends)
        copy = pltpu.make_async_remote_copy(
            src_ref=src, dst_ref=dst, send_sem=send_sem.at[k], recv_sem=recv_sem.at[k],
            device_id=to, device_id_type=MESH)
        sends.append(copy)
        return copy

    def start(*groups):
        for group in groups:
            for copy in group:
                copy.start()
        return groups[0]

    def wait(copies):
        for copy in copies:
            copy.wait_recv()

    def planes(start, stop, step_body):
        def step(k, carry):
            step_body(k)
            return carry
        lax.fori_loop(start, stop, step, 0)

    lane = lax.broadcasted_iota(jnp.int32, (Y, 128), 1)
    coarse_lane = lax.broadcasted_iota(jnp.int32, (CY, 128), 1)

    def first_advance(x, at):
        v1[at, rows, lanes] = reaction(u[x], e[0, x], FINE_STEP)

    def z_select(v, zs, k):
        zs[k] = jnp.where(lane < 64, v[k, rows, 0:128], v[k, rows, Z - 128 : Z])

    def pack(v, slot):
        columns = [jnp.where(lane == 0, v[k, rows, 0:128], pltpu.roll(v[k, rows, Z - 128 : Z], 8, 1))
                   for k in zero]
        pks[slot] = jnp.transpose(jnp.concatenate(columns, axis=0))[0:8, :]

    def unpacked(slot, side):
        return jnp.transpose(jnp.concatenate([pkr[slot, side]] * 16, axis=0))

    def unpack(v, slot):
        v[near[0], rows, Z : Z + 128] = unpacked(slot, 0)[Y : 2 * Y, :]
        v[near[1], rows, Z : Z + 128] = unpacked(slot, 1)[0:Y, :]

    def send_near(v):
        return [send(v.at[zero[1], rows, lanes], v.at[near[0], rows, lanes], dev(x=R)),
                send(v.at[zero[0], rows, lanes], v.at[near[1], rows, lanes], dev(x=L))]

    def send_far(v):
        return [send(v.at[one[1], rows, lanes], v.at[far[0], rows, lanes], dev(x=R)),
                send(v.at[one[0], rows, lanes], v.at[far[1], rows, lanes], dev(x=L))]

    def send_corner_rows(v):
        out = []
        for mine, theirs, x in ((zero[1], near[0], R), (zero[0], near[1], L)):
            out.append(send(v.at[mine, Y - 1 : Y, lanes], v.at[theirs, Y + 7 : Y + 8, lanes], dev(x=x, y=U)))
            out.append(send(v.at[mine, 0:1, lanes], v.at[theirs, Y : Y + 1, lanes], dev(x=x, y=D)))
        return out

    def send_packed(slot):
        return [send(pks.at[slot], pkr.at[slot, 0], dev(x=R, z=Q)),
                send(pks.at[slot], pkr.at[slot, 1], dev(x=L, z=Q))]

    def send_sides(v, zs, start, stop):
        ks = slice(start, stop)
        ring = slice(Z, Z + 128)
        return [
            send(v.at[ks, Y - 2 : Y, lanes], v.at[ks, Y + 6 : Y + 8, lanes], dev(y=U)),
            send(v.at[ks, 0:2, lanes], v.at[ks, Y : Y + 2, lanes], dev(y=D)),
            send(zs.at[ks, Y - 2 : Y], v.at[ks, Y + 6 : Y + 8, ring], dev(y=U, z=Q)),
            send(zs.at[ks, 0:2], v.at[ks, Y : Y + 2, ring], dev(y=D, z=Q)),
            send(zs.at[ks], v.at[ks, rows, ring], dev(z=Q)),
        ]

    def sweep_one(v, k, below, above):
        center = v[k]
        w[k] = (center + (v[above] + v[below] + ring_sum(center))) * S

    def partial_two(v, k, above):
        return v[k, rows, lanes] + (w[above, rows, lanes] + ring_sum(w[k])[rows, lanes])

    def sweep_two(v, k, below, above):
        return (partial_two(v, k, above) + w[below, rows, lanes]) * S

    for copy in first:
        copy.wait()
    for x in (0, X - 1, 1, X - 2):
        first_advance(x, place[x])
    for copy in second:
        copy.wait()
    for x in range(CX):
        total = (e[0, 2 * x] + e[0, 2 * x + 1]) + (e[1, 2 * x] + e[1, 2 * x + 1])
        for t in range(Z // 128):
            sums[t, x * Y : (x + 1) * Y, :] = total[:, t * 128 : (t + 1) * 128]
    pairs = [sums[t, pl.ds(0, CX * CY, stride=2), :] + sums[t, pl.ds(1, CX * CY, stride=2), :]
             for t in range(Z // 128)]
    halve = (lax.broadcasted_iota(jnp.int32, (Z, CZ), 0) // 2
             == lax.broadcasted_iota(jnp.int32, (Z, CZ), 1)).astype(jnp.float32)
    noise = 0.125 * jnp.dot(jnp.concatenate(pairs, axis=1), halve,
                            precision=lax.Precision.HIGHEST, preferred_element_type=jnp.float32)
    c[2 : CX + 2, 0:CY, 0:CZ] = reaction(cs[...], noise.reshape(CX, CY, CZ), COARSE_STEP)
    columns = [jnp.where(coarse_lane == 0, c[k, 0:CY, 0:CZ], pltpu.roll(c[k, 0:CY, 0:CZ], 8, 1))
               for k in (2, CX + 1)]
    pks[2] = jnp.transpose(jnp.concatenate(columns * 2, axis=0))[0:8, :]
    pack(v1, 0)

    pl.semaphore_wait(barrier, len(partners))
    inner = slice(2, CX + 2)
    coarse_x = []
    for mine, theirs, x in ((CX + 1, 1, R), (2, CX + 2, L)):
        coarse_x.append(send(c.at[mine, CY - 1 : CY, 0:CZ], c.at[theirs, CY + 7 : CY + 8, 0:CZ], dev(x=x, y=U)))
        coarse_x.append(send(c.at[mine, 0:1, 0:CZ], c.at[theirs, CY : CY + 1, 0:CZ], dev(x=x, y=D)))
    coarse_x += [
        send(c.at[CX : CX + 2, 0:CY, 0:CZ], c.at[0:2, 0:CY, 0:CZ], dev(x=R)),
        send(c.at[2:4, 0:CY, 0:CZ], c.at[CX + 2 : CX + 4, 0:CY, 0:CZ], dev(x=L)),
    ]
    coarse_x += send_packed(2)
    coarse_yz = [
        send(c.at[inner, CY - 2 : CY, 0:CZ], c.at[inner, CY + 6 : CY + 8, 0:CZ], dev(y=U)),
        send(c.at[inner, 0:2, 0:CZ], c.at[inner, CY : CY + 2, 0:CZ], dev(y=D)),
        send(c.at[inner, CY - 1 : CY, 0:CZ], c.at[inner, CY + 7 : CY + 8, CZ : 2 * CZ], dev(y=U, z=Q)),
        send(c.at[inner, 0:1, 0:CZ], c.at[inner, CY : CY + 1, CZ : 2 * CZ], dev(y=D, z=Q)),
        send(c.at[inner, 0:CY, 0:CZ], c.at[inner, 0:CY, CZ : 2 * CZ], dev(z=Q)),
    ]
    near1 = send_near(v1)
    corner1 = send_corner_rows(v1) + send_packed(0)
    far1 = send_far(v1)
    sides1 = send_sides(v1, zs1, 0, X)
    start(coarse_x, near1, corner1, far1, coarse_yz)
    third.wait()
    planes(2, X - 2, lambda x: first_advance(x, x - 1))
    planes(0, X, lambda k: z_select(v1, zs1, k))
    start(sides1)

    wait(sides1)
    planes(1, X - 3, lambda k: sweep_one(v1, k, k - 1, k + 1))
    wait(coarse_yz)
    wait(coarse_x)
    c[1, 0:CY, CZ : 2 * CZ] = unpacked(2, 0)[CY : 2 * CY, :]
    c[CX + 2, 0:CY, CZ : 2 * CZ] = unpacked(2, 1)[0:CY, :]
    for k in range(1, CX + 3):
        center = c[k]
        beside = c[k + 1] + c[k - 1] + ring_sum(center)
        cw[k - 1] = (center + COARSE_COUPLING * beside) * COARSE_SCALE
    for k in range(2, CX + 2):
        beside = cw[k, 0:CY, 0:CZ] + cw[k - 2, 0:CY, 0:CZ] + ring_sum(cw[k - 1])[0:CY, 0:CZ]
        cblk[k - 2] = (c[k, 0:CY, 0:CZ] + COARSE_COUPLING * beside) * COARSE_SCALE
    mine = co.at[:, own_y, own_z]
    gather = [send(cblk, mine, dev(y=O)), send(cblk, mine, dev(y=U)), send(cblk, mine, dev(y=D))]
    direct = send(cblk, mine, dev(z=Q))

    start(gather)
    direct.start()
    co[:, own_y, own_z] = cblk[...]

    for s in range(2):
        sweep_one(v1, one[s], zero[s], two[s])
        center = v1[zero[s]]
        p0[s] = center + (v1[one[s]] + ring_sum(center))
    for s in range(2):
        k1[s] = partial_two(v1, one[s], two[s])

    def second_advance(k):
        v2[k, rows, lanes] = reaction(sweep_two(v1, k, k - 1, k + 1), e[1, k + 1], FINE_STEP)

    planes(1, X - 3, second_advance)

    ends = (0, X - 1)
    nexts = (1, X - 2)
    wait(near1)
    for s in range(2):
        outer = (p0[s, rows, lanes] + v1[near[s], rows, lanes]) * S
        v2[one[s], rows, lanes] = reaction((k1[s] + outer) * S, e[1, nexts[s]], FINE_STEP)
    far2 = start(send_far(v2))
    planes(0, X - 2, lambda k: z_select(v2, zs2, k))
    inside2 = start(send_sides(v2, zs2, 0, X - 2))


    wait(corner1)
    unpack(v1, 0)
    for s in range(2):
        outside = v1[near[s]]
        w[zero[s]] = (p0[s] + outside) * S
        beyond = (outside + ring_sum(outside))[rows, lanes] + v1[zero[s], rows, lanes]
        k0[s] = partial_two(v1, zero[s], one[s]) + beyond * S
    wait(far1)
    for s in range(2):
        total = (k0[s] + v1[far[s], rows, lanes] * S) * S
        v2[zero[s], rows, lanes] = reaction(total, e[1, ends[s]], FINE_STEP)
    corner2 = start(send_corner_rows(v2))
    near2 = start(send_near(v2))
    pack(v2, 1)
    corner2 = corner2 + start(send_packed(1))
    for k in zero:
        z_select(v2, zs2, k)
    outside2 = start(send_sides(v2, zs2, X - 2, X))

    wait(inside2)
    planes(1, X - 3, lambda k: sweep_one(v2, k, k - 1, k + 1))

    def finish(k):
        fo[k + 1] = sweep_two(v2, k, k - 1, k + 1)

    planes(2, X - 4, finish)

    passed = []

    def pass_on(copy, owner):
        copy.wait_recv()
        block = co.at[:, pl.ds(pl.multiple_of(owner * CY, 8), CY), own_z]
        passed.append(send(block, block, dev(z=Q)))
        passed[-1].start()

    pass_on(gather[1], D)
    pass_on(gather[2], U)

    wait(outside2)
    three = (2, X - 5)
    for s in range(2):
        sweep_one(v2, one[s], zero[s], two[s])
        center = v2[zero[s]]
        p0[s] = center + (v2[one[s]] + ring_sum(center))
    for s in range(2):
        fo[place_of(two[s], X)] = sweep_two(v2, two[s], one[s], three[s])
        k1[s] = partial_two(v2, one[s], two[s]) + p0[s, rows, lanes] * S
        k0[s] = (v2[zero[s], rows, lanes] + w[one[s], rows, lanes]
                 + (ring_sum(p0[s])[rows, lanes] + v2[zero[s], rows, lanes]) * S)
    pass_on(gather[0], O)
    wait(far2)
    for s in range(2):
        k0[s] = k0[s] + v2[far[s], rows, lanes] * S
    wait(corner2)
    unpack(v2, 1)
    wait(near2)
    for s in range(2):
        outside = v2[near[s]]
        middle = outside[rows, lanes]
        fo[nexts[s]] = (k1[s] + middle * S) * S
        fo[ends[s]] = (k0[s] + (2.0 * ring_sum(outside)[rows, lanes] + middle) * S) * S

    direct.wait_recv()
    wait(passed)
    for copy in sends:
        copy.wait_send()


def place_of(k, X):
    return k + 1


def write_out(fine, coarse, fine_hbm, coarse_hbm, sems):
    copies = []
    for src, dst in ((fine, fine_hbm), (coarse, coarse_hbm)):
        half = src.shape[0] // 2
        for k in range(2):
            part = slice(k * half, (k + 1) * half)
            copies.append(pltpu.make_async_copy(src.at[part], dst.at[part], sems.at[len(copies)]))
    for copy in copies:
        copy.start()
    for copy in copies:
        copy.wait()


N_MESSAGES = 64


def body(sizes, fine_start, increments, coarse_start):
    X, Y, Z = fine_start.shape
    CX, CY, CZ = X // 2, Y // 2, Z // 2
    f32 = jnp.float32
    any_space = pl.BlockSpec(memory_space=pl.ANY)
    in_vmem = pl.BlockSpec(memory_space=pltpu.VMEM)
    fine, coarse = pl.pallas_call(
        functools.partial(kernel, sizes),
        out_shape=(pltpu.VMEM((X, Y, Z), f32), pltpu.VMEM(coarse_start.shape, f32)),
        in_specs=[any_space] * 3,
        out_specs=(in_vmem, in_vmem),
        scratch_shapes=[
            pltpu.VMEM((X, Y, Z), f32),
            pltpu.VMEM((2, X, Y, Z), f32),
            pltpu.VMEM((CX, CY, CZ), f32),
            pltpu.VMEM((X + 4, Y + 8, Z + 128), f32),
            pltpu.VMEM((X + 4, Y + 8, Z + 128), f32),
            pltpu.VMEM((X, Y + 8, Z + 128), f32),
            pltpu.VMEM((2, Y + 8, Z + 128), f32),
            pltpu.VMEM((2, Y, Z), f32),
            pltpu.VMEM((2, Y, Z), f32),
            pltpu.VMEM((X, Y, 128), f32),
            pltpu.VMEM((X, Y, 128), f32),
            pltpu.VMEM((3, 8, 128), f32),
            pltpu.VMEM((3, 2, 8, 128), f32),
            pltpu.VMEM((Z // 128, CX * Y, 128), f32),
            pltpu.VMEM((CX + 4, CY + 8, 2 * CZ), f32),
            pltpu.VMEM((CX + 2, CY + 8, 2 * CZ), f32),
            pltpu.VMEM((CX, CY, CZ), f32),
            pltpu.SemaphoreType.DMA((8,)),
            pltpu.SemaphoreType.DMA((N_MESSAGES,)),
            pltpu.SemaphoreType.DMA((N_MESSAGES,)),
        ],
        compiler_params=pltpu.CompilerParams(collective_id=0, has_side_effects=True),
    )(fine_start, increments, coarse_start)
    fine = pltpu.with_memory_space_constraint(fine, pltpu.VMEM)
    coarse = pltpu.with_memory_space_constraint(coarse, pltpu.VMEM)
    return pl.pallas_call(
        write_out,
        out_shape=(jax.ShapeDtypeStruct(fine_start.shape, f32),
                   jax.ShapeDtypeStruct(coarse_start.shape, f32)),
        in_specs=[in_vmem, in_vmem],
        out_specs=(any_space, any_space),
        scratch_shapes=[pltpu.SemaphoreType.DMA((4,))],
    )(fine, coarse)


def solution(mesh):
    sizes = tuple(mesh.shape[name] for name in ("gx", "gy", "gz"))
    return jax.shard_map(
        functools.partial(body, sizes),
        mesh=mesh,
        in_specs=(
            P(("pairs", "gx"), "gy", "gz"),
            P(None, ("pairs", "gx"), "gy", "gz"),
            P(("pairs", "gx"), None, None),
        ),
        out_specs=(P(("pairs", "gx"), "gy", "gz"), P(("pairs", "gx"), None, None)),
        check_vma=False,
    )
```

```python
import functools

import jax
import jax.numpy as jnp
from jax import lax
from jax.experimental import pallas as pl
from jax.experimental.pallas import tpu as pltpu
from jax.sharding import PartitionSpec as P

MESH = pl.DeviceIdType.MESH
NOISE = 0.3
FINE_STEP = 0.2
COARSE_STEP = 0.4
COARSE_COUPLING = 0.5
S = 1.0 / 7.0
COARSE_SCALE = 1.0 / 4.0


def reaction(state, forcing, step):
    return state + step * (state - state * state * state) + NOISE * forcing


def ring_sum(center):
    rows, lanes = center.shape
    beside = pltpu.roll(center, rows - 1, 0) + pltpu.roll(center, 1, 0)
    return beside + (pltpu.roll(center, lanes - 1, 1) + pltpu.roll(center, 1, 1))


def kernel(sizes, u_hbm, e_hbm, cs_hbm, fo, co, u, e, cs, v1, v2, w, p0, k0, k1, zs1, zs2, pks, pkr,
           sums, c, cw, cblk, load_sem, send_sem, recv_sem):
    n_gx, n_gy, n_gz = sizes
    X, Y, Z = u.shape
    CX, CY, CZ = cs.shape
    me_x, me_y, me_z = lax.axis_index("gx"), lax.axis_index("gy"), lax.axis_index("gz")
    R, L = lax.rem(me_x + 1, n_gx), lax.rem(me_x + n_gx - 1, n_gx)
    U, D = lax.rem(me_y + 1, n_gy), lax.rem(me_y + n_gy - 1, n_gy)
    O = lax.rem(me_y + 2, n_gy)
    Q = lax.rem(me_z + 1, n_gz)
    one, zero, near, far = (X - 4, X - 3), (X - 2, X - 1), (X, X + 1), (X + 2, X + 3)
    two, three = (0, X - 5), (1, X - 6)
    place = {1: X - 4, X - 2: X - 3, 0: X - 2, X - 1: X - 1}
    place.update({x: x - 2 for x in range(2, X - 2)})
    rows, lanes = slice(0, Y), slice(0, Z)

    def dev(x=None, y=None, z=None):
        return {"gx": me_x if x is None else x, "gy": me_y if y is None else y,
                "gz": me_z if z is None else z}

    loads = []

    def load(src, dst):
        copy = pltpu.make_async_copy(src, dst, load_sem.at[len(loads)])
        copy.start()
        loads.append(copy)
        return copy

    barrier = pltpu.get_barrier_semaphore()
    partners = [dev(x=R, y=U), dev(x=R, y=D), dev(x=L, y=U), dev(x=L, y=D), dev(y=O),
                dev(x=R, z=Q), dev(x=L, z=Q), dev(x=R), dev(x=L),
                dev(y=U, z=Q), dev(y=D, z=Q), dev(y=U), dev(y=D), dev(z=Q)]
    for partner in partners:
        pl.semaphore_signal(barrier, inc=1, device_id=partner, device_id_type=MESH)

    own_y = pl.ds(pl.multiple_of(me_y * CY, 8), CY)
    own_z = pl.ds(pl.multiple_of(me_z * CZ, 128), CZ)
    first = [load(e_hbm.at[0], e.at[0]), load(e_hbm.at[1], e.at[1]),
             load(cs_hbm.at[:, own_y, own_z], cs)]
    second = [load(u_hbm.at[0:2], u.at[0:2]), load(u_hbm.at[X - 2 : X], u.at[X - 2 : X])]
    third = load(u_hbm.at[2 : X - 2], u.at[2 : X - 2])

    sends = []

    def send(src, dst, to):
        k = len(sends)
        copy = pltpu.make_async_remote_copy(
            src_ref=src, dst_ref=dst, send_sem=send_sem.at[k], recv_sem=recv_sem.at[k],
            device_id=to, device_id_type=MESH)
        sends.append(copy)
        return copy

    def start(*groups):
        for group in groups:
            for copy in group:
                copy.start()
        return groups[0]

    def wait(copies):
        for copy in copies:
            copy.wait_recv()

    def planes(start, stop, step_body):
        def step(k, carry):
            step_body(k)
            return carry
        lax.fori_loop(start, stop, step, 0)

    lane = lax.broadcasted_iota(jnp.int32, (Y, 128), 1)
    coarse_lane = lax.broadcasted_iota(jnp.int32, (CY, 128), 1)

    def first_advance(x, at):
        v1[at, rows, lanes] = reaction(u[x], e[0, x], FINE_STEP)

    def z_select(v, zs, k):
        zs[k] = jnp.where(lane < 64, v[k, rows, 0:128], v[k, rows, Z - 128 : Z])

    def pack(v, slot):
        columns = [jnp.where(lane == 0, v[k, rows, 0:128], pltpu.roll(v[k, rows, Z - 128 : Z], 8, 1))
                   for k in zero]
        pks[slot] = jnp.transpose(jnp.concatenate(columns, axis=0))[0:8, :]

    def unpacked(slot, side):
        return jnp.transpose(jnp.concatenate([pkr[slot, side]] * 16, axis=0))

    def unpack(v, slot):
        v[near[0], rows, Z : Z + 128] = unpacked(slot, 0)[Y : 2 * Y, :]
        v[near[1], rows, Z : Z + 128] = unpacked(slot, 1)[0:Y, :]

    def send_near(v, part):
        return [send(v.at[zero[1], part, lanes], v.at[near[0], part, lanes], dev(x=R)),
                send(v.at[zero[0], part, lanes], v.at[near[1], part, lanes], dev(x=L))]

    def send_far(v, part):
        return [send(v.at[one[1], part, lanes], v.at[far[0], part, lanes], dev(x=R)),
                send(v.at[one[0], part, lanes], v.at[far[1], part, lanes], dev(x=L))]

    def send_corner_rows(v, half):
        mine, theirs, y = ((0, Y, D), (Y - 1, Y + 7, U))[half]
        return [
            send(v.at[zero[1], mine : mine + 1, lanes], v.at[near[0], theirs : theirs + 1, lanes], dev(x=R, y=y)),
            send(v.at[zero[0], mine : mine + 1, lanes], v.at[near[1], theirs : theirs + 1, lanes], dev(x=L, y=y)),
        ]

    M = Y // 2
    halves = (slice(0, M), slice(M, Y))

    def widened(ref, k, half):
        if half:
            return ref[k, M - 8 : Y + 8, :]
        return jnp.concatenate([ref[k, Y : Y + 8, :], ref[k, 0 : M + 8, :]], axis=0)

    def send_packed(slot):
        return [send(pks.at[slot], pkr.at[slot, 0], dev(x=R, z=Q)),
                send(pks.at[slot], pkr.at[slot, 1], dev(x=L, z=Q))]

    def send_sides(v, zs, start, stop):
        ks = slice(start, stop)
        ring = slice(Z, Z + 128)
        return [
            send(v.at[ks, Y - 2 : Y, lanes], v.at[ks, Y + 6 : Y + 8, lanes], dev(y=U)),
            send(v.at[ks, 0:2, lanes], v.at[ks, Y : Y + 2, lanes], dev(y=D)),
            send(zs.at[ks, Y - 2 : Y], v.at[ks, Y + 6 : Y + 8, ring], dev(y=U, z=Q)),
            send(zs.at[ks, 0:2], v.at[ks, Y : Y + 2, ring], dev(y=D, z=Q)),
            send(zs.at[ks], v.at[ks, rows, ring], dev(z=Q)),
        ]

    def sweep_one(v, k, below, above):
        center = v[k]
        w[k] = (center + (v[above] + v[below] + ring_sum(center))) * S

    def partial_two(v, k, above):
        return v[k, rows, lanes] + (w[above, rows, lanes] + ring_sum(w[k])[rows, lanes])

    def sweep_two(v, k, below, above):
        return (partial_two(v, k, above) + w[below, rows, lanes]) * S

    for copy in first:
        copy.wait()
    for x in range(CX):
        total = (e[0, 2 * x] + e[0, 2 * x + 1]) + (e[1, 2 * x] + e[1, 2 * x + 1])
        for t in range(Z // 128):
            sums[t, x * Y : (x + 1) * Y, :] = total[:, t * 128 : (t + 1) * 128]
    pairs = [sums[t, pl.ds(0, CX * CY, stride=2), :] + sums[t, pl.ds(1, CX * CY, stride=2), :]
             for t in range(Z // 128)]
    halve = (lax.broadcasted_iota(jnp.int32, (Z, CZ), 0) // 2
             == lax.broadcasted_iota(jnp.int32, (Z, CZ), 1)).astype(jnp.float32)
    noise = 0.125 * jnp.dot(jnp.concatenate(pairs, axis=1), halve,
                            precision=lax.Precision.HIGHEST, preferred_element_type=jnp.float32)
    c[2 : CX + 2, 0:CY, 0:CZ] = reaction(cs[...], noise.reshape(CX, CY, CZ), COARSE_STEP)
    columns = [jnp.where(coarse_lane == 0, c[k, 0:CY, 0:CZ], pltpu.roll(c[k, 0:CY, 0:CZ], 8, 1))
               for k in (2, CX + 1)]
    pks[2] = jnp.transpose(jnp.concatenate(columns * 2, axis=0))[0:8, :]
    for copy in second:
        copy.wait()
    for x in (0, X - 1, 1, X - 2):
        first_advance(x, place[x])
    pack(v1, 0)
    pl.semaphore_wait(barrier, len(partners))
    inner = slice(2, CX + 2)
    coarse_x = []
    for mine, theirs, x in ((CX + 1, 1, R), (2, CX + 2, L)):
        coarse_x.append(send(c.at[mine, CY - 1 : CY, 0:CZ], c.at[theirs, CY + 7 : CY + 8, 0:CZ], dev(x=x, y=U)))
        coarse_x.append(send(c.at[mine, 0:1, 0:CZ], c.at[theirs, CY : CY + 1, 0:CZ], dev(x=x, y=D)))
    coarse_x += [
        send(c.at[CX : CX + 2, 0:CY, 0:CZ], c.at[0:2, 0:CY, 0:CZ], dev(x=R)),
        send(c.at[2:4, 0:CY, 0:CZ], c.at[CX + 2 : CX + 4, 0:CY, 0:CZ], dev(x=L)),
    ]
    coarse_x += send_packed(2)
    coarse_yz = [
        send(c.at[inner, CY - 2 : CY, 0:CZ], c.at[inner, CY + 6 : CY + 8, 0:CZ], dev(y=U)),
        send(c.at[inner, 0:2, 0:CZ], c.at[inner, CY : CY + 2, 0:CZ], dev(y=D)),
        send(c.at[inner, CY - 1 : CY, 0:CZ], c.at[inner, CY + 7 : CY + 8, CZ : 2 * CZ], dev(y=U, z=Q)),
        send(c.at[inner, 0:1, 0:CZ], c.at[inner, CY : CY + 1, CZ : 2 * CZ], dev(y=D, z=Q)),
        send(c.at[inner, 0:CY, 0:CZ], c.at[inner, 0:CY, CZ : 2 * CZ], dev(z=Q)),
    ]
    near1 = [send_near(v1, slice(0, M + 8)), send_near(v1, slice(M + 8, Y))]
    corner1 = send_corner_rows(v1, 0) + send_corner_rows(v1, 1) + send_packed(0)
    far1 = [send_far(v1, half) for half in halves]
    sides1 = send_sides(v1, zs1, 0, X)
    start(coarse_x, near1[0], corner1, far1[0], near1[1], far1[1], coarse_yz)
    third.wait()
    planes(2, X - 2, lambda x: first_advance(x, x - 2))
    planes(0, X, lambda k: z_select(v1, zs1, k))
    start(sides1)

    H, G = COARSE_COUPLING, COARSE_SCALE
    own = (slice(0, CY), slice(0, CZ))
    ends_c, nexts_c, near_c, far_c = (2, CX + 1), (3, CX), (1, CX + 2), (0, CX + 3)
    wait(coarse_yz)
    for k in range(3, CX + 1):
        cw[k] = (c[k] + H * (c[k + 1] + c[k - 1] + ring_sum(c[k]))) * G
    kept = []
    for s in range(2):
        end, inside = ends_c[s], nexts_c[s]
        part = c[end] + H * (c[inside] + ring_sum(c[end]))
        inner_one = cw[inside]
        beyond = cw[nexts_c[1 - s], 0:CY, 0:CZ]
        next_sum = c[inside, 0:CY, 0:CZ] + H * (ring_sum(inner_one)[own] + beyond + G * part[own])
        end_sum = c[end, 0:CY, 0:CZ] + H * (inner_one[own] + G * (ring_sum(part)[own] + H * c[end, 0:CY, 0:CZ]))
        kept.append((next_sum, end_sum))
    wait(coarse_x)
    for s in range(2):
        c[near_c[s], 0:CY, CZ : 2 * CZ] = unpacked(2, s)[(1 - s) * CY : (2 - s) * CY, :]
    for s in range(2):
        outside = c[near_c[s]]
        middle = outside[own]
        next_sum, end_sum = kept[s]
        cblk[nexts_c[s] - 2] = (next_sum + (H * H * G) * middle) * G
        spread = 2.0 * H * ring_sum(outside)[own] + middle + H * c[far_c[s], 0:CY, 0:CZ]
        cblk[ends_c[s] - 2] = (end_sum + (H * G) * spread) * G
    mine = co.at[:, own_y, own_z]
    gather = [send(cblk, mine, dev(y=O)), send(cblk, mine, dev(y=U)), send(cblk, mine, dev(y=D))]
    direct = send(cblk, mine, dev(z=Q))

    start(gather)
    direct.start()
    co[:, own_y, own_z] = cblk[...]

    wait(sides1)
    for x in range(2, X - 2):
        sweep_one(v1, place[x], place[x - 1], place[x + 1])
    for s in range(2):
        sweep_one(v1, one[s], zero[s], two[s])
        center = v1[zero[s]]
        p0[s] = center + (v1[one[s]] + ring_sum(center))
    for s in range(2):
        k1[s] = partial_two(v1, one[s], two[s])

    for x in range(2, X - 2):
        total = sweep_two(v1, place[x], place[x - 1], place[x + 1])
        v2[place[x], rows, lanes] = reaction(total, e[1, x], FINE_STEP)
    planes(0, X - 4, lambda k: z_select(v2, zs2, k))
    inside2 = start(send_sides(v2, zs2, 0, X - 4))

    ends = (0, X - 1)
    nexts = (1, X - 2)
    early = list(sends)
    far2, near2, corner2 = [], [], []
    for half in range(2):
        part = halves[half]
        wait(near1[half])
        for s in range(2):
            outer = (p0[s, part, lanes] + v1[near[s], part, lanes]) * S
            v2[one[s], part, lanes] = reaction((k1[s, part] + outer) * S, e[1, nexts[s], part], FINE_STEP)
        far2 += start(send_far(v2, part))
        if half == 0:
            wait(corner1)
            unpack(v1, 0)
        for s in range(2):
            outside = widened(v1, near[s], half)
            first_sweep = (widened(p0, s, half) + outside) * S
            beyond = (outside + ring_sum(outside))[8 : M + 8, lanes] + v1[zero[s], part, lanes]
            within = w[one[s], part, lanes] + ring_sum(first_sweep)[8 : M + 8, lanes]
            k0[s, part] = v1[zero[s], part, lanes] + within + beyond * S
        wait(far1[half])
        for s in range(2):
            total = (k0[s, part] + v1[far[s], part, lanes] * S) * S
            v2[zero[s], part, lanes] = reaction(total, e[1, ends[s], part], FINE_STEP)
        corner2 += start(send_corner_rows(v2, half))
        near2 += start(send_near(v2, part))
    pack(v2, 1)
    corner2 += start(send_packed(1))
    planes(X - 4, X, lambda k: z_select(v2, zs2, k))
    outside2 = start(send_sides(v2, zs2, X - 4, X))

    wait(inside2)
    for s in range(2):
        k = two[s]
        beside = v2[one[s], rows, lanes] + v2[three[s], rows, lanes] + ring_sum(v2[k])[rows, lanes]
        w[k, rows, lanes] = (v2[k, rows, lanes] + beside) * S
    for x in range(3, X - 3):
        sweep_one(v2, place[x], place[x - 1], place[x + 1])

    for x in range(3, X - 3):
        fo[x] = sweep_two(v2, place[x], place[x - 1], place[x + 1])

    passed = []

    def pass_on(copy, owner):
        copy.wait_recv()
        block = co.at[:, pl.ds(pl.multiple_of(owner * CY, 8), CY), own_z]
        passed.append(send(block, block, dev(z=Q)))
        passed[-1].start()

    pass_on(gather[0], O)
    pass_on(gather[1], D)
    pass_on(gather[2], U)

    wait(outside2)
    for s in range(2):
        k = two[s]
        center = v2[k]
        swept = (center + (v2[one[s]] + v2[three[s]] + ring_sum(center))) * S
        w[k, :, Z : Z + 128] = swept[:, Z : Z + 128]
        w[k, Y : Y + 8, lanes] = swept[Y : Y + 8, lanes]
    for s in range(2):
        sweep_one(v2, one[s], zero[s], two[s])
        center = v2[zero[s]]
        p0[s] = center + (v2[one[s]] + ring_sum(center))
    for s in range(2):
        fo[(2, X - 3)[s]] = sweep_two(v2, two[s], one[s], three[s])
        k1[s] = partial_two(v2, one[s], two[s]) + p0[s, rows, lanes] * S
        k0[s] = (v2[zero[s], rows, lanes] + w[one[s], rows, lanes]
                 + (ring_sum(p0[s])[rows, lanes] + v2[zero[s], rows, lanes]) * S)
    for copy in early:
        copy.wait_send()
    wait(far2)
    for s in range(2):
        k0[s] = k0[s] + v2[far[s], rows, lanes] * S
    wait(corner2)
    unpack(v2, 1)
    wait(near2)
    for s in range(2):
        outside = v2[near[s]]
        middle = outside[rows, lanes]
        fo[nexts[s]] = (k1[s] + middle * S) * S
        fo[ends[s]] = (k0[s] + (2.0 * ring_sum(outside)[rows, lanes] + middle) * S) * S

    direct.wait_recv()
    wait(passed)
    for copy in sends[len(early):]:
        copy.wait_send()


def write_out(fine, coarse, fine_hbm, coarse_hbm, sems):
    copies = []
    for src, dst in ((fine, fine_hbm), (coarse, coarse_hbm)):
        for k in range(4):
            size = src.shape[0] // 4
            part = slice(k * size, (k + 1) * size)
            copies.append(pltpu.make_async_copy(src.at[part], dst.at[part], sems.at[len(copies)]))
    for copy in copies:
        copy.start()
    for copy in copies:
        copy.wait()


N_MESSAGES = 64


def body(sizes, fine_start, increments, coarse_start):
    X, Y, Z = fine_start.shape
    CX, CY, CZ = X // 2, Y // 2, Z // 2
    f32 = jnp.float32
    any_space = pl.BlockSpec(memory_space=pl.ANY)
    in_vmem = pl.BlockSpec(memory_space=pltpu.VMEM)
    fine, coarse = pl.pallas_call(
        functools.partial(kernel, sizes),
        out_shape=(pltpu.VMEM((X, Y, Z), f32), pltpu.VMEM(coarse_start.shape, f32)),
        in_specs=[any_space] * 3,
        out_specs=(in_vmem, in_vmem),
        scratch_shapes=[
            pltpu.VMEM((X, Y, Z), f32),
            pltpu.VMEM((2, X, Y, Z), f32),
            pltpu.VMEM((CX, CY, CZ), f32),
            pltpu.VMEM((X + 4, Y + 8, Z + 128), f32),
            pltpu.VMEM((X + 4, Y + 8, Z + 128), f32),
            pltpu.VMEM((X, Y + 8, Z + 128), f32),
            pltpu.VMEM((2, Y + 8, Z + 128), f32),
            pltpu.VMEM((2, Y, Z), f32),
            pltpu.VMEM((2, Y, Z), f32),
            pltpu.VMEM((X, Y, 128), f32),
            pltpu.VMEM((X, Y, 128), f32),
            pltpu.VMEM((3, 8, 128), f32),
            pltpu.VMEM((3, 2, 8, 128), f32),
            pltpu.VMEM((Z // 128, CX * Y, 128), f32),
            pltpu.VMEM((CX + 4, CY + 8, 2 * CZ), f32),
            pltpu.VMEM((CX + 2, CY + 8, 2 * CZ), f32),
            pltpu.VMEM((CX, CY, CZ), f32),
            pltpu.SemaphoreType.DMA((8,)),
            pltpu.SemaphoreType.DMA((N_MESSAGES,)),
            pltpu.SemaphoreType.DMA((N_MESSAGES,)),
        ],
        compiler_params=pltpu.CompilerParams(collective_id=0, has_side_effects=True),
    )(fine_start, increments, coarse_start)
    fine = pltpu.with_memory_space_constraint(fine, pltpu.VMEM)
    coarse = pltpu.with_memory_space_constraint(coarse, pltpu.VMEM)
    return pl.pallas_call(
        write_out,
        out_shape=(jax.ShapeDtypeStruct(fine_start.shape, f32),
                   jax.ShapeDtypeStruct(coarse_start.shape, f32)),
        in_specs=[in_vmem, in_vmem],
        out_specs=(any_space, any_space),
        scratch_shapes=[pltpu.SemaphoreType.DMA((8,))],
    )(fine, coarse)


def solution(mesh):
    sizes = tuple(mesh.shape[name] for name in ("gx", "gy", "gz"))
    return jax.shard_map(
        functools.partial(body, sizes),
        mesh=mesh,
        in_specs=(
            P(("pairs", "gx"), "gy", "gz"),
            P(None, ("pairs", "gx"), "gy", "gz"),
            P(("pairs", "gx"), None, None),
        ),
        out_specs=(P(("pairs", "gx"), "gy", "gz"), P(("pairs", "gx"), None, None)),
        check_vma=False,
    )
```

```python
import functools

import jax
import jax.numpy as jnp
from jax import lax
from jax.experimental import pallas as pl
from jax.experimental.pallas import tpu as pltpu
from jax.sharding import PartitionSpec as P

MESH = pl.DeviceIdType.MESH
NOISE = 0.3
FINE_STEP = 0.2
COARSE_STEP = 0.4
COARSE_COUPLING = 0.5
S = 1.0 / 7.0
COARSE_SCALE = 1.0 / 4.0


def reaction(state, forcing, step):
    return state + step * (state - state * state * state) + NOISE * forcing


def ring_sum(center):
    rows, lanes = center.shape
    beside = pltpu.roll(center, rows - 1, 0) + pltpu.roll(center, 1, 0)
    return beside + (pltpu.roll(center, lanes - 1, 1) + pltpu.roll(center, 1, 1))


def kernel(sizes, u_hbm, e_hbm, cs_hbm, fo, co, u, e, cs, v1, v2, w, p0, k0, k1, zs1, zs2, pks, pkr,
           sums, c, cw, cblk, load_sem, send_sem, recv_sem):
    n_gx, n_gy, n_gz = sizes
    X, Y, Z = u.shape
    CX, CY, CZ = cs.shape
    me_x, me_y, me_z = lax.axis_index("gx"), lax.axis_index("gy"), lax.axis_index("gz")
    R, L = lax.rem(me_x + 1, n_gx), lax.rem(me_x + n_gx - 1, n_gx)
    U, D = lax.rem(me_y + 1, n_gy), lax.rem(me_y + n_gy - 1, n_gy)
    O = lax.rem(me_y + 2, n_gy)
    Q = lax.rem(me_z + 1, n_gz)
    one, zero, near, far = (X - 4, X - 3), (X - 2, X - 1), (X, X + 1), (X + 2, X + 3)
    two, three = (0, X - 5), (1, X - 6)
    place = {1: X - 4, X - 2: X - 3, 0: X - 2, X - 1: X - 1}
    place.update({x: x - 2 for x in range(2, X - 2)})
    rows, lanes = slice(0, Y), slice(0, Z)

    def dev(x=None, y=None, z=None):
        return {"gx": me_x if x is None else x, "gy": me_y if y is None else y,
                "gz": me_z if z is None else z}

    loads = []

    def load(src, dst):
        copy = pltpu.make_async_copy(src, dst, load_sem.at[len(loads)])
        copy.start()
        loads.append(copy)
        return copy

    barrier = pltpu.get_barrier_semaphore()
    partners = [dev(x=R, y=U), dev(x=R, y=D), dev(x=L, y=U), dev(x=L, y=D), dev(y=O),
                dev(x=R, z=Q), dev(x=L, z=Q), dev(x=R), dev(x=L),
                dev(y=U, z=Q), dev(y=D, z=Q), dev(y=U), dev(y=D), dev(z=Q)]
    for partner in partners:
        pl.semaphore_signal(barrier, inc=1, device_id=partner, device_id_type=MESH)

    own_y = pl.ds(pl.multiple_of(me_y * CY, 8), CY)
    own_z = pl.ds(pl.multiple_of(me_z * CZ, 128), CZ)
    first = [load(e_hbm.at[0], e.at[0]), load(e_hbm.at[1], e.at[1]),
             load(cs_hbm.at[:, own_y, own_z], cs)]
    second = [load(u_hbm.at[0:2], u.at[0:2]), load(u_hbm.at[X - 2 : X], u.at[X - 2 : X])]
    third = load(u_hbm.at[2 : X - 2], u.at[2 : X - 2])

    sends = []

    def send(src, dst, to):
        k = len(sends)
        copy = pltpu.make_async_remote_copy(
            src_ref=src, dst_ref=dst, send_sem=send_sem.at[k], recv_sem=recv_sem.at[k],
            device_id=to, device_id_type=MESH)
        sends.append(copy)
        return copy

    def start(*groups):
        for group in groups:
            for copy in group:
                copy.start()
        return groups[0]

    def wait(copies):
        for copy in copies:
            copy.wait_recv()

    def planes(start, stop, step_body):
        def step(k, carry):
            step_body(k)
            return carry
        lax.fori_loop(start, stop, step, 0)

    lane = lax.broadcasted_iota(jnp.int32, (Y, 128), 1)
    coarse_lane = lax.broadcasted_iota(jnp.int32, (CY, 128), 1)

    def first_advance(x, at):
        v1[at, rows, lanes] = reaction(u[x], e[0, x], FINE_STEP)

    def z_select(v, zs, k):
        zs[k] = jnp.where(lane < 64, v[k, rows, 0:128], v[k, rows, Z - 128 : Z])

    def pack(v, slot):
        columns = [jnp.where(lane == 0, v[k, rows, 0:128], pltpu.roll(v[k, rows, Z - 128 : Z], 8, 1))
                   for k in zero]
        pks[slot] = jnp.transpose(jnp.concatenate(columns, axis=0))[0:8, :]

    def unpacked(slot, side):
        return jnp.transpose(jnp.concatenate([pkr[slot, side]] * 16, axis=0))

    def unpack(v, slot):
        v[near[0], rows, Z : Z + 128] = unpacked(slot, 0)[Y : 2 * Y, :]
        v[near[1], rows, Z : Z + 128] = unpacked(slot, 1)[0:Y, :]

    def send_near(v, part):
        return [send(v.at[zero[1], part, lanes], v.at[near[0], part, lanes], dev(x=R)),
                send(v.at[zero[0], part, lanes], v.at[near[1], part, lanes], dev(x=L))]

    def send_far(v, part):
        return [send(v.at[one[1], part, lanes], v.at[far[0], part, lanes], dev(x=R)),
                send(v.at[one[0], part, lanes], v.at[far[1], part, lanes], dev(x=L))]

    def send_corner_rows(v, half):
        mine, theirs, y = ((0, Y, D), (Y - 1, Y + 7, U))[half]
        return [
            send(v.at[zero[1], mine : mine + 1, lanes], v.at[near[0], theirs : theirs + 1, lanes], dev(x=R, y=y)),
            send(v.at[zero[0], mine : mine + 1, lanes], v.at[near[1], theirs : theirs + 1, lanes], dev(x=L, y=y)),
        ]

    M = Y // 2
    halves = (slice(0, M), slice(M, Y))

    def widened(ref, k, half):
        if half:
            return ref[k, M - 8 : Y + 8, :]
        return jnp.concatenate([ref[k, Y : Y + 8, :], ref[k, 0 : M + 8, :]], axis=0)

    def send_packed(slot):
        return [send(pks.at[slot], pkr.at[slot, 0], dev(x=R, z=Q)),
                send(pks.at[slot], pkr.at[slot, 1], dev(x=L, z=Q))]

    def send_sides(v, zs, start, stop):
        ks = slice(start, stop)
        ring = slice(Z, Z + 128)
        return [
            send(v.at[ks, Y - 2 : Y, lanes], v.at[ks, Y + 6 : Y + 8, lanes], dev(y=U)),
            send(v.at[ks, 0:2, lanes], v.at[ks, Y : Y + 2, lanes], dev(y=D)),
            send(zs.at[ks, Y - 2 : Y], v.at[ks, Y + 6 : Y + 8, ring], dev(y=U, z=Q)),
            send(zs.at[ks, 0:2], v.at[ks, Y : Y + 2, ring], dev(y=D, z=Q)),
            send(zs.at[ks], v.at[ks, rows, ring], dev(z=Q)),
        ]

    def sweep_one(v, k, below, above):
        center = v[k]
        w[k] = (center + (v[above] + v[below] + ring_sum(center))) * S

    def partial_two(v, k, above):
        return v[k, rows, lanes] + (w[above, rows, lanes] + ring_sum(w[k])[rows, lanes])

    def sweep_two(v, k, below, above):
        return (partial_two(v, k, above) + w[below, rows, lanes]) * S

    for copy in first:
        copy.wait()
    for x in range(CX):
        total = (e[0, 2 * x] + e[0, 2 * x + 1]) + (e[1, 2 * x] + e[1, 2 * x + 1])
        for t in range(Z // 128):
            sums[t, x * Y : (x + 1) * Y, :] = total[:, t * 128 : (t + 1) * 128]
    pairs = [sums[t, pl.ds(0, CX * CY, stride=2), :] + sums[t, pl.ds(1, CX * CY, stride=2), :]
             for t in range(Z // 128)]
    halve = (lax.broadcasted_iota(jnp.int32, (Z, CZ), 0) // 2
             == lax.broadcasted_iota(jnp.int32, (Z, CZ), 1)).astype(jnp.float32)
    noise = 0.125 * jnp.dot(jnp.concatenate(pairs, axis=1), halve,
                            precision=lax.Precision.HIGHEST, preferred_element_type=jnp.float32)
    c[2 : CX + 2, 0:CY, 0:CZ] = reaction(cs[...], noise.reshape(CX, CY, CZ), COARSE_STEP)
    columns = [jnp.where(coarse_lane == 0, c[k, 0:CY, 0:CZ], pltpu.roll(c[k, 0:CY, 0:CZ], 8, 1))
               for k in (2, CX + 1)]
    pks[2] = jnp.transpose(jnp.concatenate(columns * 2, axis=0))[0:8, :]
    for copy in second:
        copy.wait()
    for x in (0, X - 1, 1, X - 2):
        first_advance(x, place[x])
    pack(v1, 0)
    pl.semaphore_wait(barrier, len(partners))
    inner = slice(2, CX + 2)
    coarse_x = []
    for mine, theirs, x in ((CX + 1, 1, R), (2, CX + 2, L)):
        coarse_x.append(send(c.at[mine, CY - 1 : CY, 0:CZ], c.at[theirs, CY + 7 : CY + 8, 0:CZ], dev(x=x, y=U)))
        coarse_x.append(send(c.at[mine, 0:1, 0:CZ], c.at[theirs, CY : CY + 1, 0:CZ], dev(x=x, y=D)))
    coarse_x += [
        send(c.at[CX : CX + 2, 0:CY, 0:CZ], c.at[0:2, 0:CY, 0:CZ], dev(x=R)),
        send(c.at[2:4, 0:CY, 0:CZ], c.at[CX + 2 : CX + 4, 0:CY, 0:CZ], dev(x=L)),
    ]
    coarse_x += send_packed(2)
    coarse_yz = [
        send(c.at[inner, CY - 2 : CY, 0:CZ], c.at[inner, CY + 6 : CY + 8, 0:CZ], dev(y=U)),
        send(c.at[inner, 0:2, 0:CZ], c.at[inner, CY : CY + 2, 0:CZ], dev(y=D)),
        send(c.at[inner, CY - 1 : CY, 0:CZ], c.at[inner, CY + 7 : CY + 8, CZ : 2 * CZ], dev(y=U, z=Q)),
        send(c.at[inner, 0:1, 0:CZ], c.at[inner, CY : CY + 1, CZ : 2 * CZ], dev(y=D, z=Q)),
        send(c.at[inner, 0:CY, 0:CZ], c.at[inner, 0:CY, CZ : 2 * CZ], dev(z=Q)),
    ]
    near1 = [send_near(v1, slice(0, M + 8)), send_near(v1, slice(M + 8, Y))]
    corner1 = send_corner_rows(v1, 0) + send_corner_rows(v1, 1) + send_packed(0)
    far1 = [send_far(v1, half) for half in halves]
    sides1 = send_sides(v1, zs1, 0, X)
    start(coarse_x, near1[0], corner1, far1[0], near1[1], far1[1], coarse_yz)
    third.wait()
    planes(2, X - 2, lambda x: first_advance(x, x - 2))
    planes(0, X, lambda k: z_select(v1, zs1, k))
    start(sides1)

    H, G = COARSE_COUPLING, COARSE_SCALE
    own = (slice(0, CY), slice(0, CZ))
    ends_c, nexts_c, near_c, far_c = (2, CX + 1), (3, CX), (1, CX + 2), (0, CX + 3)
    wait(coarse_yz)
    for k in range(3, CX + 1):
        cw[k] = (c[k] + H * (c[k + 1] + c[k - 1] + ring_sum(c[k]))) * G
    kept = []
    for s in range(2):
        end, inside = ends_c[s], nexts_c[s]
        part = c[end] + H * (c[inside] + ring_sum(c[end]))
        inner_one = cw[inside]
        beyond = cw[nexts_c[1 - s], 0:CY, 0:CZ]
        next_sum = c[inside, 0:CY, 0:CZ] + H * (ring_sum(inner_one)[own] + beyond + G * part[own])
        end_sum = c[end, 0:CY, 0:CZ] + H * (inner_one[own] + G * (ring_sum(part)[own] + H * c[end, 0:CY, 0:CZ]))
        kept.append((next_sum, end_sum))
    wait(coarse_x)
    for s in range(2):
        c[near_c[s], 0:CY, CZ : 2 * CZ] = unpacked(2, s)[(1 - s) * CY : (2 - s) * CY, :]
    for s in range(2):
        outside = c[near_c[s]]
        middle = outside[own]
        next_sum, end_sum = kept[s]
        cblk[nexts_c[s] - 2] = (next_sum + (H * H * G) * middle) * G
        spread = 2.0 * H * ring_sum(outside)[own] + middle + H * c[far_c[s], 0:CY, 0:CZ]
        cblk[ends_c[s] - 2] = (end_sum + (H * G) * spread) * G
    mine = co.at[:, own_y, own_z]
    gather = [send(cblk, mine, dev(y=O)), send(cblk, mine, dev(y=U)), send(cblk, mine, dev(y=D))]
    direct = send(cblk, mine, dev(z=Q))

    start(gather)
    direct.start()
    co[:, own_y, own_z] = cblk[...]

    wait(sides1)
    for x in range(2, X - 2):
        sweep_one(v1, place[x], place[x - 1], place[x + 1])
    for s in range(2):
        sweep_one(v1, one[s], zero[s], two[s])
        center = v1[zero[s]]
        p0[s] = center + (v1[one[s]] + ring_sum(center))
    for s in range(2):
        k1[s] = partial_two(v1, one[s], two[s])

    for x in range(2, X - 2):
        total = sweep_two(v1, place[x], place[x - 1], place[x + 1])
        v2[place[x], rows, lanes] = reaction(total, e[1, x], FINE_STEP)
    planes(0, X - 4, lambda k: z_select(v2, zs2, k))
    inside2 = start(send_sides(v2, zs2, 0, X - 4))

    ends = (0, X - 1)
    nexts = (1, X - 2)
    early = list(sends)
    far2, near2, corner2 = [], [], []
    for half in range(2):
        part = halves[half]
        wait(near1[half])
        for s in range(2):
            outer = (p0[s, part, lanes] + v1[near[s], part, lanes]) * S
            v2[one[s], part, lanes] = reaction((k1[s, part] + outer) * S, e[1, nexts[s], part], FINE_STEP)
        far2 += start(send_far(v2, part))
        if half == 0:
            wait(corner1)
            unpack(v1, 0)
        for s in range(2):
            outside = widened(v1, near[s], half)
            first_sweep = (widened(p0, s, half) + outside) * S
            beyond = (outside + ring_sum(outside))[8 : M + 8, lanes] + v1[zero[s], part, lanes]
            within = w[one[s], part, lanes] + ring_sum(first_sweep)[8 : M + 8, lanes]
            k0[s, part] = v1[zero[s], part, lanes] + within + beyond * S
        wait(far1[half])
        for s in range(2):
            total = (k0[s, part] + v1[far[s], part, lanes] * S) * S
            v2[zero[s], part, lanes] = reaction(total, e[1, ends[s], part], FINE_STEP)
        edge, plane = send_corner_rows(v2, half), send_near(v2, part)
        start(*((edge, plane) if half else (plane, edge)))
        corner2 += edge
        near2 += plane
    pack(v2, 1)
    corner2 += start(send_packed(1))
    planes(X - 4, X, lambda k: z_select(v2, zs2, k))
    outside2 = start(send_sides(v2, zs2, X - 4, X))

    wait(inside2)
    for s in range(2):
        k = two[s]
        beside = v2[one[s], rows, lanes] + v2[three[s], rows, lanes] + ring_sum(v2[k])[rows, lanes]
        w[k, rows, lanes] = (v2[k, rows, lanes] + beside) * S
    for x in range(3, X - 3):
        sweep_one(v2, place[x], place[x - 1], place[x + 1])

    for x in range(3, X - 3):
        fo[x] = sweep_two(v2, place[x], place[x - 1], place[x + 1])

    passed = []

    def pass_on(copy, owner):
        copy.wait_recv()
        block = co.at[:, pl.ds(pl.multiple_of(owner * CY, 8), CY), own_z]
        passed.append(send(block, block, dev(z=Q)))
        passed[-1].start()

    pass_on(gather[0], O)
    pass_on(gather[1], D)
    pass_on(gather[2], U)

    wait(outside2)
    for s in range(2):
        k = two[s]
        center = v2[k]
        swept = (center + (v2[one[s]] + v2[three[s]] + ring_sum(center))) * S
        w[k, :, Z : Z + 128] = swept[:, Z : Z + 128]
        w[k, Y : Y + 8, lanes] = swept[Y : Y + 8, lanes]
    for s in range(2):
        sweep_one(v2, one[s], zero[s], two[s])
        center = v2[zero[s]]
        p0[s] = center + (v2[one[s]] + ring_sum(center))
    for s in range(2):
        fo[(2, X - 3)[s]] = sweep_two(v2, two[s], one[s], three[s])
        k1[s] = partial_two(v2, one[s], two[s]) + p0[s, rows, lanes] * S
        k0[s] = (v2[zero[s], rows, lanes] + w[one[s], rows, lanes]
                 + (ring_sum(p0[s])[rows, lanes] + v2[zero[s], rows, lanes]) * S)
    for copy in early:
        copy.wait_send()
    wait(far2)
    for s in range(2):
        k0[s] = k0[s] + v2[far[s], rows, lanes] * S
    wait(corner2)
    unpack(v2, 1)
    wait(near2)
    for s in range(2):
        outside = v2[near[s]]
        middle = outside[rows, lanes]
        fo[nexts[s]] = (k1[s] + middle * S) * S
        fo[ends[s]] = (k0[s] + (2.0 * ring_sum(outside)[rows, lanes] + middle) * S) * S

    direct.wait_recv()
    wait(passed)
    for copy in sends[len(early):]:
        copy.wait_send()


def write_out(fine, coarse, fine_hbm, coarse_hbm, sems):
    copies = []
    for src, dst in ((fine, fine_hbm), (coarse, coarse_hbm)):
        for k in range(4):
            size = src.shape[0] // 4
            part = slice(k * size, (k + 1) * size)
            copies.append(pltpu.make_async_copy(src.at[part], dst.at[part], sems.at[len(copies)]))
    for copy in copies:
        copy.start()
    for copy in copies:
        copy.wait()


N_MESSAGES = 64


def body(sizes, fine_start, increments, coarse_start):
    X, Y, Z = fine_start.shape
    CX, CY, CZ = X // 2, Y // 2, Z // 2
    f32 = jnp.float32
    any_space = pl.BlockSpec(memory_space=pl.ANY)
    in_vmem = pl.BlockSpec(memory_space=pltpu.VMEM)
    fine, coarse = pl.pallas_call(
        functools.partial(kernel, sizes),
        out_shape=(pltpu.VMEM((X, Y, Z), f32), pltpu.VMEM(coarse_start.shape, f32)),
        in_specs=[any_space] * 3,
        out_specs=(in_vmem, in_vmem),
        scratch_shapes=[
            pltpu.VMEM((X, Y, Z), f32),
            pltpu.VMEM((2, X, Y, Z), f32),
            pltpu.VMEM((CX, CY, CZ), f32),
            pltpu.VMEM((X + 4, Y + 8, Z + 128), f32),
            pltpu.VMEM((X + 4, Y + 8, Z + 128), f32),
            pltpu.VMEM((X, Y + 8, Z + 128), f32),
            pltpu.VMEM((2, Y + 8, Z + 128), f32),
            pltpu.VMEM((2, Y, Z), f32),
            pltpu.VMEM((2, Y, Z), f32),
            pltpu.VMEM((X, Y, 128), f32),
            pltpu.VMEM((X, Y, 128), f32),
            pltpu.VMEM((3, 8, 128), f32),
            pltpu.VMEM((3, 2, 8, 128), f32),
            pltpu.VMEM((Z // 128, CX * Y, 128), f32),
            pltpu.VMEM((CX + 4, CY + 8, 2 * CZ), f32),
            pltpu.VMEM((CX + 2, CY + 8, 2 * CZ), f32),
            pltpu.VMEM((CX, CY, CZ), f32),
            pltpu.SemaphoreType.DMA((8,)),
            pltpu.SemaphoreType.DMA((N_MESSAGES,)),
            pltpu.SemaphoreType.DMA((N_MESSAGES,)),
        ],
        compiler_params=pltpu.CompilerParams(collective_id=0, has_side_effects=True),
    )(fine_start, increments, coarse_start)
    fine = pltpu.with_memory_space_constraint(fine, pltpu.VMEM)
    coarse = pltpu.with_memory_space_constraint(coarse, pltpu.VMEM)
    return pl.pallas_call(
        write_out,
        out_shape=(jax.ShapeDtypeStruct(fine_start.shape, f32),
                   jax.ShapeDtypeStruct(coarse_start.shape, f32)),
        in_specs=[in_vmem, in_vmem],
        out_specs=(any_space, any_space),
        scratch_shapes=[pltpu.SemaphoreType.DMA((8,))],
    )(fine, coarse)


def solution(mesh):
    sizes = tuple(mesh.shape[name] for name in ("gx", "gy", "gz"))
    return jax.shard_map(
        functools.partial(body, sizes),
        mesh=mesh,
        in_specs=(
            P(("pairs", "gx"), "gy", "gz"),
            P(None, ("pairs", "gx"), "gy", "gz"),
            P(("pairs", "gx"), None, None),
        ),
        out_specs=(P(("pairs", "gx"), "gy", "gz"), P(("pairs", "gx"), None, None)),
        check_vma=False,
    )
```
